32 devices in a mesh: dp: 4 (over y, z), tp: 8 (over x, core).
Axes of the slice: x: 4, y: 2, z: 2, core: 2. Of those that a mesh axis runs over, the one named last changes fastest.
The devices are a block of a 4x4x8 slice.
Arguments:
- x_tokens: bfloat16 [4, 2048, 2048], P('dp', 'tp'), parts along dimension 0
- ln1_gain: float32 [2, 2048], replicated
- ln1_bias: float32 [2, 2048], replicated
- ln2_gain: float32 [2, 2048], replicated
- ln2_bias: float32 [2, 2048], replicated
- w_qkv: bfloat16 [2, 2048, 3, 16, 128], P(None, None, None, 'tp')
- w_out: bfloat16 [2, 16, 128, 2048], P(None, 'tp')
- b_out: float32 [2, 2048], replicated
- w_up: bfloat16 [2, 2048, 8192], P(None, None, 'tp')
- b_up: float32 [2, 8192], P(None, 'tp')
- w_down: bfloat16 [2, 8192, 2048], P(None, 'tp')
- b_down: float32 [2, 2048], replicated
Outputs:
- output: bfloat16 [4, 2048, 2048], P('dp', 'tp'), parts along dimension 0
There are 4 independent parts. The reference program is written for one: setup_inputs(seed, part) draws one part's arguments, and reference() takes and returns one part's arrays. A program takes and returns all parts, laid end to end along the dimension named above; an argument that names none is the same for every part.
All inputs are finite; a program needn't handle non-finite values.
Results may differ from the reference program's by a relative error of at most 0.0104569.
Values are sent between devices in bfloat16 or wider.
A program may use at most 768 MiB of HBM per device.

```python
import math
import jax
import jax.numpy as jnp
from jax import lax

BATCH = 1
SEQ_LEN = 2048
D_MODEL = 2048
HEADS = 16
HEAD_DIM = 128
D_FF = 8192
LAYERS = 2


def setup_inputs(seed: int = 0, part: int = 0) -> dict:
    base_key = jax.random.key(seed)
    part_key = jax.random.fold_in(base_key, part)
    row_key, tok_key = jax.random.split(part_key)
    keys = jax.random.split(base_key, 11)
    row_scale = 0.5 + jax.random.uniform(row_key, (BATCH, SEQ_LEN, 1), jnp.float32)
    tokens = jax.random.normal(tok_key, (BATCH, SEQ_LEN, D_MODEL), jnp.float32) * row_scale
    qk_gain = (math.log(SEQ_LEN) / 2.0) ** 0.25
    attn_level = math.sqrt((1.0 + 0.5 * math.log(SEQ_LEN)) / math.sqrt(SEQ_LEN))
    out_gain = 0.5 / attn_level
    proj_gain = jnp.array([qk_gain, qk_gain, 1.0], jnp.float32).reshape(1, 1, 3, 1, 1)
    vec_shape = (LAYERS, D_MODEL)
    w_qkv = jax.random.normal(keys[4], (LAYERS, D_MODEL, 3, HEADS, HEAD_DIM), jnp.float32) * proj_gain * D_MODEL ** -0.5
    w_out = jax.random.normal(keys[5], (LAYERS, HEADS, HEAD_DIM, D_MODEL), jnp.float32) * (out_gain * D_MODEL ** -0.5)
    w_up = jax.random.normal(keys[7], (LAYERS, D_MODEL, D_FF), jnp.float32) * D_MODEL ** -0.5
    w_down = jax.random.normal(keys[9], (LAYERS, D_FF, D_MODEL), jnp.float32) * (0.8 * D_FF ** -0.5)
    return {
        "x_tokens": tokens.astype(jnp.bfloat16),
        "ln1_gain": 1.0 + 0.2 * jax.random.normal(keys[0], vec_shape, jnp.float32),
        "ln1_bias": 0.2 * jax.random.normal(keys[1], vec_shape, jnp.float32),
        "ln2_gain": 1.0 + 0.2 * jax.random.normal(keys[2], vec_shape, jnp.float32),
        "ln2_bias": 0.2 * jax.random.normal(keys[3], vec_shape, jnp.float32),
        "w_qkv": w_qkv.astype(jnp.bfloat16),
        "w_out": w_out.astype(jnp.bfloat16),
        "b_out": 0.2 * jax.random.normal(keys[6], vec_shape, jnp.float32),
        "w_up": w_up.astype(jnp.bfloat16),
        "b_up": 0.3 * jax.random.normal(keys[8], (LAYERS, D_FF), jnp.float32),
        "w_down": w_down.astype(jnp.bfloat16),
        "b_down": 0.2 * jax.random.normal(keys[10], vec_shape, jnp.float32),
    }


def layer_norm(resid, gain, shift):
    row_mean = jnp.mean(resid, axis=-1, keepdims=True)
    centered = resid - row_mean
    variance = jnp.mean(centered * centered, axis=-1, keepdims=True)
    return (centered * lax.rsqrt(variance + 1e-5) * gain + shift).astype(jnp.bfloat16)


def attention_head(head_parts):
    queries, keys_all, values_all = head_parts
    scores = jnp.einsum("bqe,bke->bqk", queries.astype(jnp.float32), keys_all.astype(jnp.float32)) / math.sqrt(HEAD_DIM)
    positions = jnp.arange(SEQ_LEN)
    causal = positions[:, None] >= positions[None, :]
    scores = jnp.where(causal, scores, -1e30)
    attn_probs = jax.nn.softmax(scores, axis=-1).astype(jnp.bfloat16)
    return jnp.einsum("bqk,bke->bqe", attn_probs.astype(jnp.float32), values_all.astype(jnp.float32)).astype(jnp.bfloat16)


def layer_step(resid, params):
    ln1_gain, ln1_bias, ln2_gain, ln2_bias, w_qkv, w_out, b_out, w_up, b_up, w_down, b_down = params
    normed = layer_norm(resid, ln1_gain, ln1_bias)
    qkv_proj = jnp.dot(normed.reshape(BATCH * SEQ_LEN, D_MODEL), w_qkv.reshape(D_MODEL, 3 * HEADS * HEAD_DIM), preferred_element_type=jnp.float32).astype(jnp.bfloat16)
    qkv_proj = qkv_proj.reshape(BATCH, SEQ_LEN, 3, HEADS, HEAD_DIM)
    heads_first = jnp.transpose(qkv_proj, (2, 3, 0, 1, 4))
    attn_heads = lax.map(attention_head, (heads_first[0], heads_first[1], heads_first[2]))
    attn_out = jnp.einsum("hbse,hed->bsd", attn_heads.astype(jnp.float32), w_out.astype(jnp.float32))
    resid = resid + (attn_out + b_out)
    normed_mlp = layer_norm(resid, ln2_gain, ln2_bias)
    pre_act = jnp.dot(normed_mlp.reshape(BATCH * SEQ_LEN, D_MODEL), w_up, preferred_element_type=jnp.float32) + b_up
    hidden = jax.nn.gelu(pre_act, approximate=True).astype(jnp.bfloat16)
    mlp_out = jnp.dot(hidden, w_down, preferred_element_type=jnp.float32).reshape(BATCH, SEQ_LEN, D_MODEL)
    resid = resid + (mlp_out + b_down)
    return resid, None


def reference(x_tokens, ln1_gain, ln1_bias, ln2_gain, ln2_bias, w_qkv, w_out, b_out, w_up, b_up, w_down, b_down):
    params = (ln1_gain, ln1_bias, ln2_gain, ln2_bias, w_qkv, w_out, b_out, w_up, b_up, w_down, b_down)
    resid, _ = lax.scan(layer_step, x_tokens.astype(jnp.float32), params)
    return resid.astype(jnp.bfloat16)
```

```python
import functools
import math
import jax
import jax.numpy as jnp
from jax import lax
from jax.experimental import pallas as pl
from jax.experimental.pallas import tpu as pltpu
from jax.sharding import PartitionSpec as P

F32 = jnp.float32
BF16 = jnp.bfloat16
MESH = pl.DeviceIdType.MESH
OPP, RIGHT, LEFT, OWN = range(4)


def pick(i, values):
    out = values[0]
    for n in range(1, len(values)):
        out = jnp.where(i == n, values[n], out)
    return out


def decoder(tp_size, layers, heads, head_dim,
            x_ref, g1_ref, s1_ref, g2_ref, s2_ref, bo_ref, bu_ref, bd_ref,
            wqkv_hbm, wout_hbm, wup_hbm, wdown_hbm,
            y_ref,
            hid, qkv, resid, acc, pst, prv, snd, rcv, scores, mask, mlp, att,
            wqkv, wout, wup, wdown,
            wsem, ag_ss, ag_rs, rs_ss, rs_rs):
    chips = tp_size // 2
    rows, width = x_ref.shape
    half, quarter = rows // 2, rows // 4
    hd = heads * head_dim
    scale = 1.0 / math.sqrt(head_dim)
    me = lax.axis_index("tp")
    chip = me // 2
    core = lax.rem(me, 2)
    right = lax.rem(me + 2, tp_size)
    left = lax.rem(me + tp_size - 2, tp_size)
    mate = me + 1 - 2 * core
    chip_of = [lax.rem(chip + 2, chips), lax.rem(chip + 1, chips), lax.rem(chip + chips - 1, chips), chip]
    top, low = pl.ds(0, quarter), pl.ds(quarter, quarter)
    mine, other = pl.ds(0, half), pl.ds(half, half)

    def remote(src, dst, ss, rs, s, k, to):
        return pltpu.make_async_remote_copy(src, dst, ss.at[s, k], rs.at[s, k], device_id={"tp": to}, device_id_type=MESH)

    def gather_copy(s, k):
        if k < 3:
            blk = hid.at[chip if k < 2 else chip_of[LEFT], s, top if k == 1 else low]
            return remote(blk, blk, ag_ss, ag_rs, s, k, right)
        if k < 6:
            blk = hid.at[chip if k < 5 else chip_of[RIGHT], s, low if k == 4 else top]
            return remote(blk, blk, ag_ss, ag_rs, s, k, left)
        c = chip_of[k - 6]
        return remote(hid.at[c, s, mine], hid.at[c, s, other], ag_ss, ag_rs, s, k, mate)

    def gather_send(s):
        for k in (0, 3, 6 + OWN, 1, 4):
            gather_copy(s, k).start()

    def gather_first(s):
        gather_copy(s, 0).wait_recv()
        gather_copy(s, 2).start()
        gather_copy(s, 3).wait_recv()
        gather_copy(s, 5).start()

    def gather_second(s):
        gather_copy(s, 1).wait_recv()
        gather_copy(s, 6 + LEFT).start()
        gather_copy(s, 4).wait_recv()
        gather_copy(s, 6 + RIGHT).start()

    def gather_third(s):
        gather_copy(s, 2).wait_recv()
        gather_copy(s, 5).wait_recv()
        gather_copy(s, 6 + OPP).start()

    def gather_mate(s, kind):
        gather_copy(s, 6 + kind).wait_recv()

    def sum_copy(s, k):
        if k < 6:
            return remote(snd.at[s, k], rcv.at[s, k], rs_ss, rs_rs, s, k, right if k < 3 else left)
        return remote(pst.at[s, k - 6], prv.at[s, k - 6], rs_ss, rs_rs, s, k, mate)

    def mate_send(s, kind):
        remote(pst.at[s, kind], prv.at[s, kind], rs_ss, rs_rs, s, 6 + kind, mate).start()

    step = 16

    def combine(s, kind, r0, dst, extra):
        @pl.loop(0, quarter // step)
        def _(t):
            at = pl.ds(pl.multiple_of(r0 + t * step, step), step)
            at0 = pl.ds(pl.multiple_of(t * step, step), step)
            total = acc[s, kind, at, :] + prv[s, kind, at, :].astype(F32)
            if extra is not None:
                total = total + rcv[s, extra, at0, :].astype(F32)
            snd[s, dst, at0, :] = total.astype(BF16)

    def send_opp(s):
        for k in (2, 5, 6, 7, 8, 9):
            gather_copy(s, k).wait_send()
        sum_copy(s, 6 + OPP).wait_recv()
        combine(s, OPP, quarter, 0, None)
        sum_copy(s, 0).start()
        combine(s, OPP, 0, 3, None)
        sum_copy(s, 3).start()

    def send_near(s):
        sum_copy(s, 6 + RIGHT).wait_recv()
        combine(s, RIGHT, 0, 1, None)
        sum_copy(s, 1).start()
        sum_copy(s, 6 + LEFT).wait_recv()
        combine(s, LEFT, quarter, 4, None)
        sum_copy(s, 4).start()

    def send_through(s):
        sum_copy(s, 0).wait_recv()
        combine(s, RIGHT, quarter, 2, 0)
        sum_copy(s, 2).start()
        sum_copy(s, 3).wait_recv()
        combine(s, LEFT, 0, 5, 3)
        sum_copy(s, 5).start()

    def norm_row(s, at0, r, gain_ref, shift_ref, layer):
        mean = jnp.mean(r, axis=-1, keepdims=True)
        centered = r - mean
        var = jnp.mean(centered * centered, axis=-1, keepdims=True)
        normed = centered * lax.rsqrt(var + 1e-5) * gain_ref[pl.ds(layer, 1), :] + shift_ref[pl.ds(layer, 1), :]
        hid[chip, s, at0, :] = normed.astype(BF16)

    def finish(s, layer, bias_ref, gain_ref, shift_ref, next_layer, last):
        for k in (1, 2, 4, 5, 6 + OWN):
            sum_copy(s, k).wait_recv()
        for k in range(10):
            sum_copy(s, k).wait_send()
        for k in (0, 1, 3, 4):
            gather_copy(s, k).wait_send()
        for part, a, b in ((0, 1, 5), (1, 2, 4)):
            @pl.loop(0, quarter // step)
            def _(t):
                at0 = pl.ds(pl.multiple_of(t * step, step), step)
                at = pl.ds(pl.multiple_of(part * quarter + t * step, step), step)
                rat = pl.ds(pl.multiple_of(s * half + part * quarter + t * step, step), step)
                total = acc[s, OWN, at, :] + prv[s, OWN, at, :].astype(F32)
                total = total + (rcv[s, a, at0, :].astype(F32) + rcv[s, b, at0, :].astype(F32))
                r = resid[rat, :] + (total + bias_ref[pl.ds(layer, 1), :])
                resid[rat, :] = r
                if last is None:
                    norm_row(s, at, r, gain_ref, shift_ref, next_layer)
                else:
                    @pl.when(last)
                    def _():
                        y_ref[rat, :] = r.astype(BF16)

                    @pl.when(jnp.logical_not(last))
                    def _():
                        norm_row(s, at, r, gain_ref, shift_ref, next_layer)
        if last is None:
            gather_send(s)
        else:
            @pl.when(jnp.logical_not(last))
            def _():
                gather_send(s)

    def block_at(s):
        return pl.ds(pl.multiple_of(s * rows, rows), rows)

    def do_qkv(s, d):
        @pl.loop(0, 3)
        def _(n):
            cols = pl.ds(pl.multiple_of(n * hd, hd), hd)
            qkv[d, block_at(s), cols] = jnp.dot(hid[d, s], wqkv[:, cols], preferred_element_type=F32).astype(BF16)

    def project(s, kind, lhs_ref, w_ref):
        tile = min(256, width)

        @pl.loop(0, width // tile)
        def _(n):
            cols = pl.ds(pl.multiple_of(n * tile, tile), tile)
            part = jnp.dot(lhs_ref[...], w_ref[:, cols], preferred_element_type=F32)
            acc[s, kind, :, cols] = part[:half]
            pst[s, kind, :, cols] = part[half:].astype(BF16)
        mate_send(s, kind)

    def do_mlp(s, d, kind, layer):
        hidden = wup.shape[1]
        tile = min(256, hidden)

        @pl.loop(0, hidden // tile)
        def _(n):
            cols = pl.ds(pl.multiple_of(n * tile, tile), tile)
            pre = jnp.dot(hid[d, s], wup[:, cols], preferred_element_type=F32) + bu_ref[pl.ds(layer, 1), cols]
            mlp[:, cols] = jax.nn.gelu(pre, approximate=True).astype(BF16)
        project(s, kind, mlp, wdown)

    def do_attention(s, d, kind):
        lanes = head_dim
        for h in range(heads):
            q = qkv[d, block_at(s), h * head_dim:(h + 1) * head_dim]

            def score(k):
                keys = qkv[k, :, hd + h * head_dim:hd + (h + 1) * head_dim]
                return lax.dot_general(q, keys, (((1,), (1,)), ((), ())), preferred_element_type=F32) * scale

            def fold(op, into, tile):
                for j in range(tile.shape[1] // lanes):
                    into = op(into, tile[:, j * lanes:(j + 1) * lanes])
                return into

            def first(k, top_so_far):
                sc = score(k)
                scores[k] = sc
                return fold(jnp.maximum, top_so_far, sc)

            peak = lax.fori_loop(0, d, first, jnp.full((rows, lanes), -1e30, F32))
            sc = jnp.where(mask[s] > 0.0, score(d), -1e30)
            scores[d] = sc
            peak = jnp.max(fold(jnp.maximum, peak, sc), axis=-1, keepdims=True)

            def second(k, total):
                e = jnp.exp(scores[k] - peak)
                scores[k] = e
                return fold(jnp.add, total, e)

            total = lax.fori_loop(0, d + 1, second, jnp.zeros((rows, lanes), F32))
            inv = 1.0 / jnp.sum(total, axis=-1, keepdims=True)

            def third(k, out):
                p = (scores[k] * inv).astype(BF16)
                vals = qkv[k, :, 2 * hd + h * head_dim:2 * hd + (h + 1) * head_dim]
                return out + jnp.dot(p, vals, preferred_element_type=F32)

            out = lax.fori_loop(0, d + 1, third, jnp.zeros((rows, head_dim), F32))
            att[:, h * head_dim:(h + 1) * head_dim] = out.astype(BF16)
        project(s, kind, att, wout)

    weights = ((wqkv_hbm, wqkv), (wout_hbm, wout), (wup_hbm, wup), (wdown_hbm, wdown))

    def weight_copy(n, layer):
        return pltpu.make_async_copy(weights[n][0].at[layer], weights[n][1], wsem.at[n])

    def next_weights(layer, which):
        @pl.when(layer + 1 < layers)
        def _():
            for n in which:
                weight_copy(n, layer + 1).start()

    for n in range(4):
        weight_copy(n, 0).start()

    barrier = pltpu.get_barrier_semaphore()
    for peer in (left, right, mate):
        pl.semaphore_signal(barrier, inc=1, device_id={"tp": peer}, device_id_type=MESH)
    pl.semaphore_wait(barrier, 3)

    for s in (0, 1):
        @pl.loop(0, half // step)
        def _(t):
            at = pl.ds(pl.multiple_of(t * step, step), step)
            rat = pl.ds(pl.multiple_of(s * half + t * step, step), step)
            r = x_ref[rat, :].astype(F32)
            resid[rat, :] = r
            norm_row(s, at, r, g1_ref, s1_ref, 0)
        gather_send(s)

    key = lax.broadcasted_iota(jnp.int32, (rows, 2 * rows), 1)
    key_core = jnp.where(lax.rem(key, rows) < half, core, 1 - core)
    key_at = key_core * rows + jnp.where(key < rows, 0, half) + lax.rem(key, half)
    qry = lax.broadcasted_iota(jnp.int32, (rows, 2 * rows), 0)
    qry_at = jnp.where(qry < half, core, 1 - core) * rows + lax.rem(qry, half)
    for s in (0, 1):
        mask[s] = (key_at <= qry_at + s * half).astype(F32)

    gather_order = [(OWN, 0), (LEFT, 0), (RIGHT, 0), (OPP, 0), (OWN, 1), (LEFT, 1), (RIGHT, 1), (OPP, 1)]
    sum_order = [(OPP, 0), (OPP, 1), (RIGHT, 0), (LEFT, 0), (OWN, 0), (RIGHT, 1), (LEFT, 1), (OWN, 1)]

    def run(order, before, work, after):
        @pl.loop(0, len(order))
        def _(i):
            for n in range(len(order)):
                if n in before:
                    pl.when(i == n)(before[n])
            kind = pick(i, [k for k, _ in order])
            work(pick(i, [s for _, s in order]), pick(i, [chip_of[k] for k, _ in order]), kind)
            for n in range(len(order)):
                if n in after:
                    pl.when(i == n)(after[n])

    def layer_body(layer, _):
        def arrive(extra):
            def at0():
                gather_mate(0, OWN)

            def at1():
                gather_first(0)
                gather_second(0)
                gather_mate(0, LEFT)
                gather_mate(0, RIGHT)

            def at3():
                gather_first(1)
                gather_third(0)
                gather_mate(0, OPP)

            def at4():
                gather_mate(1, OWN)

            def at5():
                gather_second(1)
                if extra:
                    send_opp(0)
                    send_near(0)
                gather_mate(1, LEFT)
                gather_mate(1, RIGHT)

            def at7():
                gather_third(1)
                gather_mate(1, OPP)
            return {0: at0, 1: at1, 3: at3, 4: at4, 5: at5, 7: at7}

        weight_copy(0, layer).wait()
        run(gather_order, arrive(False), lambda s, d, kind: do_qkv(s, d), {})
        next_weights(layer, (0,))

        weight_copy(1, layer).wait()

        def after3():
            send_near(0)
            send_through(0)

        def after6():
            send_near(1)
            send_through(1)

        run(sum_order, {}, do_attention, {0: lambda: send_opp(0), 1: lambda: send_opp(1), 3: after3, 6: after6})
        next_weights(layer, (1,))
        for s in (0, 1):
            finish(s, layer, bo_ref, g2_ref, s2_ref, layer, None)

        weight_copy(2, layer).wait()
        weight_copy(3, layer).wait()
        run(gather_order, arrive(True), lambda s, d, kind: do_mlp(s, d, kind, layer), {})
        next_weights(layer, (2, 3))
        send_through(0)
        send_opp(1)
        send_near(1)
        send_through(1)
        last = layer == layers - 1
        for s in (0, 1):
            finish(s, layer, bd_ref, g1_ref, s1_ref, jnp.minimum(layer + 1, layers - 1), last)
        return 0

    lax.fori_loop(0, layers, layer_body, 0)


def solution(mesh):
    tp_size = mesh.shape["tp"]

    def local_forward(x_local, ln1_gain, ln1_bias, ln2_gain, ln2_bias, w_qkv, w_out, b_out, w_up, b_up, w_down, b_down):
        batch, rows, width = x_local.shape
        layers, _, _, heads, head_dim = w_qkv.shape
        hidden = w_up.shape[2]
        hd = heads * head_dim
        chips = tp_size // 2
        half, quarter = rows // 2, rows // 4
        vmem = pl.BlockSpec(memory_space=pltpu.VMEM)
        anywhere = pl.BlockSpec(memory_space=pl.ANY)
        call = pl.pallas_call(
            functools.partial(decoder, tp_size, layers, heads, head_dim),
            out_shape=jax.ShapeDtypeStruct((rows, width), BF16),
            in_specs=[vmem] * 8 + [anywhere] * 4,
            out_specs=vmem,
            scratch_shapes=[
                pltpu.VMEM((chips, 2, rows, width), BF16),
                pltpu.VMEM((chips, 2 * rows, 3 * hd), BF16),
                pltpu.VMEM((rows, width), F32),
                pltpu.VMEM((2, 4, half, width), F32),
                pltpu.VMEM((2, 4, half, width), BF16),
                pltpu.VMEM((2, 4, half, width), BF16),
                pltpu.VMEM((2, 6, quarter, width), BF16),
                pltpu.VMEM((2, 6, quarter, width), BF16),
                pltpu.VMEM((chips, rows, 2 * rows), F32),
                pltpu.VMEM((2, rows, 2 * rows), F32),
                pltpu.VMEM((rows, hidden), BF16),
                pltpu.VMEM((rows, hd), BF16),
                pltpu.VMEM((width, 3 * hd), BF16),
                pltpu.VMEM((hd, width), BF16),
                pltpu.VMEM((width, hidden), BF16),
                pltpu.VMEM((hidden, width), BF16),
                pltpu.SemaphoreType.DMA((4,)),
                pltpu.SemaphoreType.DMA((2, 10)),
                pltpu.SemaphoreType.DMA((2, 10)),
                pltpu.SemaphoreType.DMA((2, 10)),
                pltpu.SemaphoreType.DMA((2, 10)),
            ],
            compiler_params=pltpu.CompilerParams(collective_id=0, has_side_effects=True, vmem_limit_bytes=64 * 1024 * 1024 - 128 * 1024),
        )
        y = call(
            x_local.reshape(rows, width), ln1_gain, ln1_bias, ln2_gain, ln2_bias, b_out, b_up, b_down,
            w_qkv.reshape(layers, width, 3 * hd), w_out.reshape(layers, hd, width), w_up, w_down,
        )
        return y.reshape(batch, rows, width)

    rows_spec = P("dp", "tp", None)
    in_specs = (rows_spec, P(), P(), P(), P(), P(None, None, None, "tp", None), P(None, "tp", None, None), P(), P(None, None, "tp"), P(None, "tp"), P(None, "tp", None), P())
    return jax.shard_map(local_forward, mesh=mesh, in_specs=in_specs, out_specs=rows_spec, check_vma=False)
```

```python
import functools
import math
import jax
import jax.numpy as jnp
from jax import lax
from jax.experimental import pallas as pl
from jax.experimental.pallas import tpu as pltpu
from jax.sharding import PartitionSpec as P

F32 = jnp.float32
BF16 = jnp.bfloat16
MESH = pl.DeviceIdType.MESH
OPP, RIGHT, LEFT, OWN = range(4)


def pick(i, values):
    out = values[0]
    for n in range(1, len(values)):
        out = jnp.where(i == n, values[n], out)
    return out


def decoder(tp_size, layers, heads, head_dim,
            x_ref, g1_ref, s1_ref, g2_ref, s2_ref, bo_ref, bu_ref, bd_ref,
            wqkv_hbm, wout_hbm, wup_hbm, wdown_hbm,
            y_ref,
            hid, qk, vt, resid, acc, pst, prv, snd, rcv, scores, mask, mlp, att,
            wraw, order_ref, wqkv, wout, wup, wdown,
            wsem, ag_ss, ag_rs, rs_ss, rs_rs):
    chips = tp_size // 2
    rows, width = x_ref.shape
    half, quarter = rows // 2, rows // 4
    hd = heads * head_dim
    scale = 1.0 / math.sqrt(head_dim)
    me = lax.axis_index("tp")
    chip = me // 2
    core = lax.rem(me, 2)
    right = lax.rem(me + 2, tp_size)
    left = lax.rem(me + tp_size - 2, tp_size)
    mate = me + 1 - 2 * core
    chip_of = [lax.rem(chip + 2, chips), lax.rem(chip + 1, chips), lax.rem(chip + chips - 1, chips), chip]
    top, low = pl.ds(0, quarter), pl.ds(quarter, quarter)
    mine, other = pl.ds(0, half), pl.ds(half, half)

    def remote(src, dst, ss, rs, s, k, to):
        return pltpu.make_async_remote_copy(src, dst, ss.at[s, k], rs.at[s, k], device_id={"tp": to}, device_id_type=MESH)

    def gather_copy(s, k):
        if k < 3:
            blk = hid.at[chip if k < 2 else chip_of[LEFT], s, top if k == 1 else low]
            return remote(blk, blk, ag_ss, ag_rs, s, k, right)
        if k < 6:
            blk = hid.at[chip if k < 5 else chip_of[RIGHT], s, low if k == 4 else top]
            return remote(blk, blk, ag_ss, ag_rs, s, k, left)
        c = chip_of[k - 6]
        return remote(hid.at[c, s, mine], hid.at[c, s, other], ag_ss, ag_rs, s, k, mate)

    def gather_send(s):
        for k in (0, 3, 6 + OWN, 1, 4):
            gather_copy(s, k).start()

    def gather_first(s):
        gather_copy(s, 0).wait_recv()
        gather_copy(s, 2).start()
        gather_copy(s, 3).wait_recv()
        gather_copy(s, 5).start()

    def gather_second(s):
        gather_copy(s, 1).wait_recv()
        gather_copy(s, 6 + LEFT).start()
        gather_copy(s, 4).wait_recv()
        gather_copy(s, 6 + RIGHT).start()

    def gather_third(s):
        gather_copy(s, 2).wait_recv()
        gather_copy(s, 5).wait_recv()
        gather_copy(s, 6 + OPP).start()

    def gather_mate(s, kind):
        gather_copy(s, 6 + kind).wait_recv()

    def sum_copy(s, k):
        if k < 6:
            return remote(snd.at[s, k], rcv.at[s, k], rs_ss, rs_rs, s, k, right if k < 3 else left)
        return remote(pst.at[s, k - 6], prv.at[s, k - 6], rs_ss, rs_rs, s, k, mate)

    def mate_send(s, kind):
        remote(pst.at[s, kind], prv.at[s, kind], rs_ss, rs_rs, s, 6 + kind, mate).start()

    step = 16

    def combine(s, kind, r0, dst, extra):
        @pl.loop(0, quarter // step)
        def _(t):
            at = pl.ds(pl.multiple_of(r0 + t * step, step), step)
            at0 = pl.ds(pl.multiple_of(t * step, step), step)
            total = acc[s, kind, at, :] + prv[s, kind, at, :].astype(F32)
            if extra is not None:
                total = total + rcv[s, extra, at0, :].astype(F32)
            snd[s, dst, at0, :] = total.astype(BF16)

    def send_opp(s):
        gather_copy(s, 6 + OPP).wait_send()
        sum_copy(s, 6 + OPP).wait_recv()
        combine(s, OPP, quarter, 0, None)
        sum_copy(s, 0).start()
        combine(s, OPP, 0, 3, None)
        sum_copy(s, 3).start()

    def send_near(s):
        sum_copy(s, 6 + RIGHT).wait_recv()
        combine(s, RIGHT, 0, 1, None)
        sum_copy(s, 1).start()
        sum_copy(s, 6 + LEFT).wait_recv()
        combine(s, LEFT, quarter, 4, None)
        sum_copy(s, 4).start()

    def send_through(s):
        for k in (2, 5, 6 + RIGHT, 6 + LEFT):
            gather_copy(s, k).wait_send()
        sum_copy(s, 0).wait_recv()
        combine(s, RIGHT, quarter, 2, 0)
        sum_copy(s, 2).start()
        sum_copy(s, 3).wait_recv()
        combine(s, LEFT, 0, 5, 3)
        sum_copy(s, 5).start()

    def norm_row(s, at0, r, gain_ref, shift_ref, layer):
        mean = jnp.mean(r, axis=-1, keepdims=True)
        centered = r - mean
        var = jnp.mean(centered * centered, axis=-1, keepdims=True)
        normed = centered * lax.rsqrt(var + 1e-5) * gain_ref[pl.ds(layer, 1), :] + shift_ref[pl.ds(layer, 1), :]
        hid[chip, s, at0, :] = normed.astype(BF16)

    def finish(s, layer, bias_ref, gain_ref, shift_ref, next_layer, last):
        for k in (1, 2, 4, 5, 6 + OWN):
            sum_copy(s, k).wait_recv()
        for k in range(10):
            sum_copy(s, k).wait_send()
        for k in (0, 1, 3, 4, 6 + OWN):
            gather_copy(s, k).wait_send()
        for part, a, b in ((0, 1, 5), (1, 2, 4)):
            @pl.loop(0, quarter // step)
            def _(t):
                at0 = pl.ds(pl.multiple_of(t * step, step), step)
                at = pl.ds(pl.multiple_of(part * quarter + t * step, step), step)
                rat = pl.ds(pl.multiple_of(s * half + part * quarter + t * step, step), step)
                total = acc[s, OWN, at, :] + prv[s, OWN, at, :].astype(F32)
                total = total + (rcv[s, a, at0, :].astype(F32) + rcv[s, b, at0, :].astype(F32))
                r = resid[rat, :] + (total + bias_ref[pl.ds(layer, 1), :])
                resid[rat, :] = r
                if last is None:
                    norm_row(s, at, r, gain_ref, shift_ref, next_layer)
                else:
                    @pl.when(last)
                    def _():
                        y_ref[rat, :] = r.astype(BF16)

                    @pl.when(jnp.logical_not(last))
                    def _():
                        norm_row(s, at, r, gain_ref, shift_ref, next_layer)
        if last is None:
            gather_send(s)
        else:
            @pl.when(jnp.logical_not(last))
            def _():
                gather_send(s)

    def block_at(s):
        return pl.ds(pl.multiple_of(s * rows, rows), rows)

    def do_qkv(s, d):
        out = jnp.dot(hid[d, s], wqkv[...], preferred_element_type=F32)
        qk[d, block_at(s), :] = out[:, :2 * hd].astype(BF16)
        vt[d, :, block_at(s)] = jnp.transpose(out[:, 2 * hd:]).astype(BF16)

    def project(s, kind, lhs_ref, w_ref):
        tile = min(1024, width)

        @pl.loop(0, width // tile)
        def _(n):
            cols = pl.ds(pl.multiple_of(n * tile, tile), tile)
            part = jnp.dot(lhs_ref[...], w_ref[:, cols], preferred_element_type=F32)
            acc[s, kind, :, cols] = part[:half]
            pst[s, kind, :, cols] = part[half:].astype(BF16)
        mate_send(s, kind)

    def do_mlp(s, d, kind, layer):
        hidden = wup.shape[1]
        tile = min(1024, hidden)

        @pl.loop(0, hidden // tile)
        def _(n):
            cols = pl.ds(pl.multiple_of(n * tile, tile), tile)
            pre = jnp.dot(hid[d, s], wup[:, cols], preferred_element_type=F32) + bu_ref[pl.ds(layer, 1), cols]
            mlp[:, cols] = jax.nn.gelu(pre, approximate=True).astype(BF16)
        project(s, kind, mlp, wdown)

    def attend(s, d):
        keys, lanes = 2 * rows, 8
        for h in range(heads):
            at = slice(h * head_dim, (h + 1) * head_dim)
            q = qk[d, block_at(s), at]
            peak = None
            for k in range(d + 1):
                sc = lax.dot_general(qk[k, :, hd + h * head_dim:hd + (h + 1) * head_dim], q, (((1,), (1,)), ((), ())), preferred_element_type=F32)
                if k == d:
                    sc = jnp.where(mask[s] > 0.0, sc, -3e38)
                scores[h, k] = sc
                top_here = jnp.max(sc.reshape(keys // lanes, lanes, rows), axis=0)
                peak = top_here if peak is None else jnp.maximum(peak, top_here)
            peak = jnp.max(peak, axis=0, keepdims=True)
            total = None
            for k in range(d + 1):
                e = jnp.exp2((scores[h, k] - peak) * (scale * math.log2(math.e)))
                scores[h, k] = e
                here = jnp.sum(e.reshape(keys // lanes, lanes, rows), axis=0)
                total = here if total is None else total + here
            inv = 1.0 / jnp.sum(total, axis=0, keepdims=True)
            out = None
            for k in range(d + 1):
                p = (scores[h, k] * inv).astype(BF16)
                here = jnp.dot(vt[k, at, :], p, preferred_element_type=F32)
                out = here if out is None else out + here
            att[:, at] = jnp.transpose(out).astype(BF16)

    def do_attention(s, d, kind):
        for n in range(chips):
            @pl.when(d == n)
            def _():
                attend(s, n)
        project(s, kind, att, wout)

    weights = ((wqkv_hbm, wraw), (wout_hbm, wout), (wup_hbm, wup), (wdown_hbm, wdown))

    def weight_copy(n, layer):
        return pltpu.make_async_copy(weights[n][0].at[layer], weights[n][1], wsem.at[n])

    def next_weights(layer, which):
        @pl.when(layer + 1 < layers)
        def _():
            for n in which:
                weight_copy(n, layer + 1).start()

    for n in range(4):
        weight_copy(n, 0).start()

    barrier = pltpu.get_barrier_semaphore()
    for peer in (left, right, mate):
        pl.semaphore_signal(barrier, inc=1, device_id={"tp": peer}, device_id_type=MESH)
    for s in (0, 1):
        @pl.loop(0, half // step)
        def _(t):
            at = pl.ds(pl.multiple_of(t * step, step), step)
            rat = pl.ds(pl.multiple_of(s * half + t * step, step), step)
            r = x_ref[rat, :].astype(F32)
            resid[rat, :] = r
            norm_row(s, at, r, g1_ref, s1_ref, 0)
        if s == 0:
            pl.semaphore_wait(barrier, 3)
        gather_send(s)

    key = lax.broadcasted_iota(jnp.int32, (2 * rows, rows), 0)
    key_core = jnp.where(lax.rem(key, rows) < half, core, 1 - core)
    key_at = key_core * rows + jnp.where(key < rows, 0, half) + lax.rem(key, half)
    qry = lax.broadcasted_iota(jnp.int32, (2 * rows, rows), 1)
    qry_at = jnp.where(qry < half, core, 1 - core) * rows + lax.rem(qry, half)
    for s in (0, 1):
        mask[s] = (key_at <= qry_at + s * half).astype(F32)

    parts = 3 * heads
    to = lax.broadcasted_iota(jnp.int32, (parts * 128, parts * 128), 0)
    come = lax.broadcasted_iota(jnp.int32, (parts * 128, parts * 128), 1)
    order_ref[...] = (come == lax.rem(to, 128) * parts + to // 128).astype(BF16)

    def sort_wqkv():
        @pl.loop(0, width // 128)
        def _(n):
            rows_in = pl.ds(pl.multiple_of(n * parts * 128, 128), parts * 128)
            rows_out = pl.ds(pl.multiple_of(n * 128, 128), 128)
            moved = jnp.dot(order_ref[...], wraw[rows_in, :], preferred_element_type=F32).astype(BF16)
            for p in range(parts):
                wqkv[rows_out, p * head_dim:(p + 1) * head_dim] = moved[p * 128:(p + 1) * 128]

    gather_order = [(OWN, 0), (LEFT, 0), (RIGHT, 0), (OWN, 1), (LEFT, 1), (RIGHT, 1), (OPP, 0), (OPP, 1)]
    sum_order = [(OPP, 0), (OPP, 1), (RIGHT, 0), (LEFT, 0), (OWN, 0), (RIGHT, 1), (LEFT, 1), (OWN, 1)]

    def run(order, before, work, after):
        @pl.loop(0, len(order))
        def _(i):
            for n in range(len(order)):
                if n in before:
                    pl.when(i == n)(before[n])
            kind = pick(i, [k for k, _ in order])
            work(pick(i, [s for _, s in order]), pick(i, [chip_of[k] for k, _ in order]), kind)
            for n in range(len(order)):
                if n in after:
                    pl.when(i == n)(after[n])

    def layer_body(layer, _):
        def arrive(extra):
            def at0():
                gather_mate(0, OWN)

            def at1():
                gather_first(0)
                gather_second(0)
                gather_mate(0, LEFT)
                gather_mate(0, RIGHT)

            def at3():
                gather_mate(1, OWN)

            def at4():
                gather_first(1)
                gather_second(1)
                gather_mate(1, LEFT)
                gather_mate(1, RIGHT)

            def at6():
                if extra:
                    send_near(0)
                gather_third(0)
                gather_mate(0, OPP)

            def at7():
                if extra:
                    send_near(1)
                gather_third(1)
                if extra:
                    send_opp(0)
                gather_mate(1, OPP)
            return {0: at0, 1: at1, 3: at3, 4: at4, 6: at6, 7: at7}

        weight_copy(0, layer).wait()
        sort_wqkv()
        next_weights(layer, (0,))
        run(gather_order, arrive(False), lambda s, d, kind: do_qkv(s, d), {})

        weight_copy(1, layer).wait()

        def after3():
            send_near(0)
            send_through(0)

        def after6():
            send_near(1)
            send_through(1)

        run(sum_order, {}, do_attention, {0: lambda: send_opp(0), 1: lambda: send_opp(1), 3: after3, 6: after6})
        next_weights(layer, (1,))
        for s in (0, 1):
            finish(s, layer, bo_ref, g2_ref, s2_ref, layer, None)

        weight_copy(2, layer).wait()
        weight_copy(3, layer).wait()
        run(gather_order, arrive(True), lambda s, d, kind: do_mlp(s, d, kind, layer), {})
        next_weights(layer, (2, 3))
        send_opp(1)
        send_through(0)
        send_through(1)
        last = layer == layers - 1
        for s in (0, 1):
            finish(s, layer, bd_ref, g1_ref, s1_ref, jnp.minimum(layer + 1, layers - 1), last)
        return 0

    lax.fori_loop(0, layers, layer_body, 0)


def solution(mesh):
    tp_size = mesh.shape["tp"]

    def local_forward(x_local, ln1_gain, ln1_bias, ln2_gain, ln2_bias, w_qkv, w_out, b_out, w_up, b_up, w_down, b_down):
        batch, rows, width = x_local.shape
        layers, _, _, heads, head_dim = w_qkv.shape
        hidden = w_up.shape[2]
        hd = heads * head_dim
        chips = tp_size // 2
        half, quarter = rows // 2, rows // 4
        vmem = pl.BlockSpec(memory_space=pltpu.VMEM)
        anywhere = pl.BlockSpec(memory_space=pl.ANY)
        call = pl.pallas_call(
            functools.partial(decoder, tp_size, layers, heads, head_dim),
            out_shape=jax.ShapeDtypeStruct((rows, width), BF16),
            in_specs=[vmem] * 8 + [anywhere] * 4,
            out_specs=vmem,
            scratch_shapes=[
                pltpu.VMEM((chips, 2, rows, width), BF16),
                pltpu.VMEM((chips, 2 * rows, 2 * hd), BF16),
                pltpu.VMEM((chips, hd, 2 * rows), BF16),
                pltpu.VMEM((rows, width), F32),
                pltpu.VMEM((2, 4, half, width), F32),
                pltpu.VMEM((2, 4, half, width), BF16),
                pltpu.VMEM((2, 4, half, width), BF16),
                pltpu.VMEM((2, 6, quarter, width), BF16),
                pltpu.VMEM((2, 6, quarter, width), BF16),
                pltpu.VMEM((heads, chips, 2 * rows, rows), F32),
                pltpu.VMEM((2, 2 * rows, rows), F32),
                pltpu.VMEM((rows, hidden), BF16),
                pltpu.VMEM((rows, hd), BF16),
                pltpu.VMEM((3 * heads * width, head_dim), BF16),
                pltpu.VMEM((3 * heads * 128, 3 * heads * 128), BF16),
                pltpu.VMEM((width, 3 * hd), BF16),
                pltpu.VMEM((hd, width), BF16),
                pltpu.VMEM((width, hidden), BF16),
                pltpu.VMEM((hidden, width), BF16),
                pltpu.SemaphoreType.DMA((4,)),
                pltpu.SemaphoreType.DMA((2, 10)),
                pltpu.SemaphoreType.DMA((2, 10)),
                pltpu.SemaphoreType.DMA((2, 10)),
                pltpu.SemaphoreType.DMA((2, 10)),
            ],
            compiler_params=pltpu.CompilerParams(collective_id=0, has_side_effects=True, vmem_limit_bytes=64 * 1024 * 1024 - 128 * 1024),
        )
        y = call(
            x_local.reshape(rows, width), ln1_gain, ln1_bias, ln2_gain, ln2_bias, b_out, b_up, b_down,
            w_qkv.reshape(layers, width * 3 * heads, head_dim), w_out.reshape(layers, hd, width), w_up, w_down,
        )
        return y.reshape(batch, rows, width)

    rows_spec = P("dp", "tp", None)
    in_specs = (rows_spec, P(), P(), P(), P(), P(None, None, None, "tp", None), P(None, "tp", None, None), P(), P(None, None, "tp"), P(None, "tp"), P(None, "tp", None), P())
    return jax.shard_map(local_forward, mesh=mesh, in_specs=in_specs, out_specs=rows_spec, check_vma=False)
```

```python
import functools
import math
import jax
import jax.numpy as jnp
from jax import lax
from jax.experimental import pallas as pl
from jax.experimental.pallas import tpu as pltpu
from jax.sharding import PartitionSpec as P

F32 = jnp.float32
BF16 = jnp.bfloat16
MESH = pl.DeviceIdType.MESH
OPP, RIGHT, LEFT, OWN = range(4)


def pick(i, values):
    out = values[0]
    for n in range(1, len(values)):
        out = jnp.where(i == n, values[n], out)
    return out


def decoder(tp_size, sharers, layers, heads, head_dim,
            x_ref, g1_ref, s1_ref, g2_ref, s2_ref, bo_ref, bu_ref, bd_ref,
            wqkv_hbm, wout_hbm, wup_hbm, wdown_hbm,
            y_ref, wg,
            hid, qk, vt, resid, acc, pst, prv, snd, rcv, scores, mask, mlp, att, heads_in,
            wraw, order_ref, wqkv, wout, wup, wdown,
            wsem, lsem, ag_ss, ag_rs, rs_ss, rs_rs, hs_ss, hs_rs, wo_ss, wo_rs):
    chips = tp_size // 2
    rows, width = x_ref.shape
    half, quarter = rows // 2, rows // 4
    hd = heads * head_dim
    scale = 1.0 / math.sqrt(head_dim)
    me = lax.axis_index("tp")
    chip = me // 2
    core = lax.rem(me, 2)
    right = lax.rem(me + 2, tp_size)
    left = lax.rem(me + tp_size - 2, tp_size)
    mate = me + 1 - 2 * core
    opposite = lax.rem(me + tp_size // 2, tp_size)
    group = lax.axis_index("dp")
    side = lax.rem(group, sharers)
    chip_of = [lax.rem(chip + 2, chips), lax.rem(chip + 1, chips), lax.rem(chip + chips - 1, chips), chip]
    top, low = pl.ds(0, quarter), pl.ds(quarter, quarter)
    mine, other = pl.ds(0, half), pl.ds(half, half)

    def remote(src, dst, ss, rs, s, k, to):
        return pltpu.make_async_remote_copy(src, dst, ss.at[s, k], rs.at[s, k], device_id={"tp": to}, device_id_type=MESH)

    def gather_copy(s, k):
        if k < 3:
            blk = hid.at[chip if k < 2 else chip_of[LEFT], s, top if k == 1 else low]
            return remote(blk, blk, ag_ss, ag_rs, s, k, right)
        if k < 6:
            blk = hid.at[chip if k < 5 else chip_of[RIGHT], s, low if k == 4 else top]
            return remote(blk, blk, ag_ss, ag_rs, s, k, left)
        c = chip_of[k - 6]
        return remote(hid.at[c, s, mine], hid.at[c, s, other], ag_ss, ag_rs, s, k, mate)

    part = hd // sharers
    piece = part // 2
    to_mate = 6 + 3 * (sharers - 1)
    wout_copies = to_mate + 4

    def wout_copy(layer, k):
        def rows_at(off, size):
            return pl.ds(pl.multiple_of(side * part + off, piece), size)

        def go(src, dst, to):
            return pltpu.make_async_remote_copy(src, dst, wo_ss.at[layer, k], wo_rs.at[layer, k], device_id=to, device_id_type=MESH)

        if k < 6:
            at = rows_at(piece if k in (0, 2, 4) else 0, piece)
            to = {"tp": right if k < 3 else left}
            if k in (2, 5):
                blk = wg.at[layer, left if k == 2 else right, at]
                return go(blk, blk, to)
            return go(wout_hbm.at[layer, at], wg.at[layer, me, at], to)
        if k < to_mate + 3:
            shard = (left, right, opposite)[k % 3]
            if k < to_mate:
                blk = wg.at[layer, shard, rows_at(0, part)]
                return go(blk, blk, {"dp": group - side + lax.rem(side + (k - 6) // 3 + 1, sharers)})
            return go(wg.at[layer, shard], wg.at[layer, shard], {"tp": mate})
        return go(wout_hbm.at[layer], wg.at[layer, me], {"tp": mate})

    def wout_begin(layer):
        for k in (0, 3, 1, 4, to_mate + 3):
            wout_copy(layer, k).start()

    def wout_pass(layer):
        for k, onward in ((0, 2), (3, 5)):
            wout_copy(layer, k).wait_recv()
            wout_copy(layer, onward).start()

    def wout_share(layer):
        for k in (1, 4, 2, 5):
            wout_copy(layer, k).wait_recv()
        for k in range(6, to_mate):
            wout_copy(layer, k).start()

    def wout_collect(layer):
        for k in range(6, to_mate):
            wout_copy(layer, k).wait_recv()
        for k in range(to_mate, to_mate + 3):
            wout_copy(layer, k).start()

    def wout_end(layer):
        for k in range(to_mate, wout_copies):
            wout_copy(layer, k).wait_recv()
        for k in range(wout_copies):
            wout_copy(layer, k).wait_send()

    others = [(OPP, 0), (RIGHT, 0), (LEFT, 0), (OPP, 1), (RIGHT, 1), (LEFT, 1), (OWN, 1)]
    seen_from = {OPP: OPP, RIGHT: LEFT, LEFT: RIGHT, OWN: OWN}

    def device_at(kind, across):
        return chip_of[kind] * 2 + (1 - core if across else core)

    def wout_load(layer, n):
        kept = pst.at[pl.ds(n * hd, hd)] if n < 4 else snd.at[pl.ds((n - 4) * hd, hd)]
        return pltpu.make_async_copy(wg.at[layer, device_at(*others[n])], kept, lsem.at[n])

    def heads_copy(s, kind, across):
        slot = 1 + others.index((seen_from[kind], across))
        k = 2 * kind + across
        return pltpu.make_async_remote_copy(
            att.at[s, kind, other if across else mine], heads_in.at[s, :, pl.ds(slot * hd, hd)],
            hs_ss.at[s, k], hs_rs.at[s, k], device_id={"tp": device_at(kind, across)}, device_id_type=MESH)

    def send_heads(s, kind):
        for across in (0, 1):
            if (kind, across) == (OWN, 0):
                heads_in[s, :, :hd] = att[s, OWN, mine, :]
            else:
                heads_copy(s, kind, across).start()

    def gather_send(s, which=(0, 3, 6 + OWN, 1, 4)):
        for k in which:
            gather_copy(s, k).start()

    def gather_first(s):
        gather_copy(s, 0).wait_recv()
        gather_copy(s, 2).start()
        gather_copy(s, 3).wait_recv()
        gather_copy(s, 5).start()

    def gather_second(s):
        gather_copy(s, 1).wait_recv()
        gather_copy(s, 6 + LEFT).start()
        gather_copy(s, 4).wait_recv()
        gather_copy(s, 6 + RIGHT).start()

    def gather_third(s):
        gather_copy(s, 2).wait_recv()
        gather_copy(s, 5).wait_recv()
        gather_copy(s, 6 + OPP).start()

    def gather_mate(s, kind):
        gather_copy(s, 6 + kind).wait_recv()

    def sum_copy(s, k):
        if k < 6:
            return remote(snd.at[pl.ds((s * 6 + k) * quarter, quarter)], rcv.at[s, k], rs_ss, rs_rs, s, k, right if k < 3 else left)
        return remote(pst.at[pl.ds((s * 4 + k - 6) * half, half)], prv.at[s, k - 6], rs_ss, rs_rs, s, k, mate)

    def staged(s, kind):
        return pl.ds(pl.multiple_of((s * 4 + kind) * half, half), half)

    def mate_send(s, kind):
        remote(pst.at[staged(s, kind)], prv.at[s, kind], rs_ss, rs_rs, s, 6 + kind, mate).start()

    step = 16

    def combine(s, kind, r0, dst, extra):
        @pl.loop(0, quarter // step)
        def _(t):
            at = pl.ds(pl.multiple_of(r0 + t * step, step), step)
            at0 = pl.ds(pl.multiple_of(t * step, step), step)
            total = acc[s, kind, at, :] + prv[s, kind, at, :].astype(F32)
            if extra is not None:
                total = total + rcv[s, extra, at0, :].astype(F32)
            snd[pl.ds(pl.multiple_of((s * 6 + dst) * quarter + t * step, step), step), :] = total.astype(BF16)

    def send_opp(s):
        gather_copy(s, 6 + OPP).wait_send()
        sum_copy(s, 6 + OPP).wait_recv()
        combine(s, OPP, quarter, 0, None)
        sum_copy(s, 0).start()
        combine(s, OPP, 0, 3, None)
        sum_copy(s, 3).start()

    def send_near(s):
        sum_copy(s, 6 + RIGHT).wait_recv()
        combine(s, RIGHT, 0, 1, None)
        sum_copy(s, 1).start()
        sum_copy(s, 6 + LEFT).wait_recv()
        combine(s, LEFT, quarter, 4, None)
        sum_copy(s, 4).start()

    def send_through(s):
        for k in (2, 5, 6 + RIGHT, 6 + LEFT):
            gather_copy(s, k).wait_send()
        sum_copy(s, 0).wait_recv()
        combine(s, RIGHT, quarter, 2, 0)
        sum_copy(s, 2).start()
        sum_copy(s, 3).wait_recv()
        combine(s, LEFT, 0, 5, 3)
        sum_copy(s, 5).start()

    def norm_row(s, at0, r, gain_ref, shift_ref, layer):
        mean = jnp.mean(r, axis=-1, keepdims=True)
        centered = r - mean
        var = jnp.mean(centered * centered, axis=-1, keepdims=True)
        normed = centered * lax.rsqrt(var + 1e-5) * gain_ref[pl.ds(layer, 1), :] + shift_ref[pl.ds(layer, 1), :]
        hid[chip, s, at0, :] = normed.astype(BF16)

    def finish(s, layer, bias_ref, gain_ref, shift_ref, next_layer, last):
        for k in (1, 2, 4, 5, 6 + OWN):
            sum_copy(s, k).wait_recv()
        for k in range(10):
            sum_copy(s, k).wait_send()
        for k in (0, 1, 3, 4, 6 + OWN):
            gather_copy(s, k).wait_send()
        for which, a, b in ((0, 1, 5), (1, 2, 4)):
            @pl.loop(0, quarter // step)
            def _(t):
                at0 = pl.ds(pl.multiple_of(t * step, step), step)
                at = pl.ds(pl.multiple_of(which * quarter + t * step, step), step)
                rat = pl.ds(pl.multiple_of(s * half + which * quarter + t * step, step), step)
                total = acc[s, OWN, at, :] + prv[s, OWN, at, :].astype(F32)
                total = total + (rcv[s, a, at0, :].astype(F32) + rcv[s, b, at0, :].astype(F32))
                r = resid[rat, :] + (total + bias_ref[pl.ds(layer, 1), :])
                resid[rat, :] = r
                if last is None:
                    norm_row(s, at, r, gain_ref, shift_ref, next_layer)
                else:
                    @pl.when(last)
                    def _():
                        y_ref[rat, :] = r.astype(BF16)

                    @pl.when(jnp.logical_not(last))
                    def _():
                        norm_row(s, at, r, gain_ref, shift_ref, next_layer)
        if last is None:
            gather_send(s)
        else:
            @pl.when(jnp.logical_not(last))
            def _():
                gather_send(s)

    def finish_attention(s, layer):
        for kind, across in others:
            heads_copy(s, kind, across).wait_recv()
        for kind, across in others:
            heads_copy(s, kind, across).wait_send()
        for k in (0, 1, 3, 4, 6 + OWN):
            gather_copy(s, k).wait_send()
        tile = min(512, width)
        mid = 5 * hd

        @pl.loop(0, width // tile)
        def _(n):
            cols = pl.ds(pl.multiple_of(n * tile, tile), tile)
            total = jnp.dot(heads_in[s, :, :hd], wout[:, cols], preferred_element_type=F32)
            total = total + jnp.dot(heads_in[s, :, hd:mid], pst[:mid - hd, cols], preferred_element_type=F32)
            total = total + jnp.dot(heads_in[s, :, mid:], snd[:tp_size * hd - mid, cols], preferred_element_type=F32)
            at = pl.ds(s * half, half)
            resid[at, cols] = resid[at, cols] + (total + bo_ref[pl.ds(layer, 1), cols])

        @pl.loop(0, half // step)
        def _(t):
            at = pl.ds(pl.multiple_of(t * step, step), step)
            norm_row(s, at, resid[pl.ds(pl.multiple_of(s * half + t * step, step), step), :], g2_ref, s2_ref, layer)

    def block_at(s):
        return pl.ds(pl.multiple_of(s * rows, rows), rows)

    def do_qkv(s, d):
        out = jnp.dot(hid[d, s], wqkv[...], preferred_element_type=F32)
        qk[d, block_at(s), :] = out[:, :2 * hd].astype(BF16)
        vt[d, :, block_at(s)] = jnp.transpose(out[:, 2 * hd:]).astype(BF16)

    def project(s, kind, lhs_ref, w_ref):
        tile = min(1024, width)

        @pl.loop(0, width // tile)
        def _(n):
            cols = pl.ds(pl.multiple_of(n * tile, tile), tile)
            total = jnp.dot(lhs_ref[...], w_ref[:, cols], preferred_element_type=F32)
            acc[s, kind, :, cols] = total[:half]
            pst[staged(s, kind), cols] = total[half:].astype(BF16)
        mate_send(s, kind)

    def do_mlp(s, d, kind, layer):
        hidden = wup.shape[1]
        tile = min(1024, hidden)

        @pl.loop(0, hidden // tile)
        def _(n):
            cols = pl.ds(pl.multiple_of(n * tile, tile), tile)
            pre = jnp.dot(hid[d, s], wup[:, cols], preferred_element_type=F32) + bu_ref[pl.ds(layer, 1), cols]
            mlp[:, cols] = jax.nn.gelu(pre, approximate=True).astype(BF16)
        project(s, kind, mlp, wdown)

    def attend(s, d, kind):
        keys, lanes = 2 * rows, 8
        for h in range(heads):
            at = slice(h * head_dim, (h + 1) * head_dim)
            q = qk[d, block_at(s), at]
            peak = None
            for k in range(d + 1):
                sc = lax.dot_general(qk[k, :, hd + h * head_dim:hd + (h + 1) * head_dim], q, (((1,), (1,)), ((), ())), preferred_element_type=F32)
                if k == d:
                    sc = jnp.where(mask[s] > 0.0, sc, -3e38)
                scores[h, k] = sc
                top_here = jnp.max(sc.reshape(keys // lanes, lanes, rows), axis=0)
                peak = top_here if peak is None else jnp.maximum(peak, top_here)
            peak = jnp.max(peak, axis=0, keepdims=True)
            total = None
            for k in range(d + 1):
                e = jnp.exp2((scores[h, k] - peak) * (scale * math.log2(math.e)))
                scores[h, k] = e
                here = jnp.sum(e.reshape(keys // lanes, lanes, rows), axis=0)
                total = here if total is None else total + here
            inv = 1.0 / jnp.sum(total, axis=0, keepdims=True)
            out = None
            for k in range(d + 1):
                p = (scores[h, k] * inv).astype(BF16)
                here = jnp.dot(vt[k, at, :], p, preferred_element_type=F32)
                out = here if out is None else out + here
            att[s, kind, :, at] = jnp.transpose(out).astype(BF16)

    def do_attention(s, d, kind):
        for n in range(chips):
            @pl.when(d == n)
            def _():
                attend(s, n, kind)

    weights = ((wqkv_hbm, wraw), (wout_hbm, wout), (wup_hbm, wup), (wdown_hbm, wdown))

    def weight_copy(n, layer):
        return pltpu.make_async_copy(weights[n][0].at[layer], weights[n][1], wsem.at[n])

    def next_weights(layer, which):
        @pl.when(layer + 1 < layers)
        def _():
            for n in which:
                weight_copy(n, layer + 1).start()

    for n in range(4):
        weight_copy(n, 0).start()

    barrier = pltpu.get_barrier_semaphore()
    for n in range(1, tp_size):
        pl.semaphore_signal(barrier, inc=1, device_id={"tp": lax.rem(me + n, tp_size)}, device_id_type=MESH)
    for n in range(1, sharers):
        pl.semaphore_signal(barrier, inc=1, device_id={"dp": group - side + lax.rem(side + n, sharers)}, device_id_type=MESH)
    for s in (0, 1):
        @pl.loop(0, half // step)
        def _(t):
            at = pl.ds(pl.multiple_of(t * step, step), step)
            rat = pl.ds(pl.multiple_of(s * half + t * step, step), step)
            r = x_ref[rat, :].astype(F32)
            resid[rat, :] = r
            norm_row(s, at, r, g1_ref, s1_ref, 0)
        if s == 0:
            pl.semaphore_wait(barrier, tp_size + sharers - 2)
        gather_send(s)

    key = lax.broadcasted_iota(jnp.int32, (2 * rows, rows), 0)
    key_core = jnp.where(lax.rem(key, rows) < half, core, 1 - core)
    key_at = key_core * rows + jnp.where(key < rows, 0, half) + lax.rem(key, half)
    qry = lax.broadcasted_iota(jnp.int32, (2 * rows, rows), 1)
    qry_at = jnp.where(qry < half, core, 1 - core) * rows + lax.rem(qry, half)
    for s in (0, 1):
        mask[s] = (key_at <= qry_at + s * half).astype(F32)

    parts = 3 * heads
    to = lax.broadcasted_iota(jnp.int32, (parts * 128, parts * 128), 0)
    come = lax.broadcasted_iota(jnp.int32, (parts * 128, parts * 128), 1)
    order_ref[...] = (come == lax.rem(to, 128) * parts + to // 128).astype(BF16)

    def sort_wqkv():
        @pl.loop(0, width // 128)
        def _(n):
            rows_in = pl.ds(pl.multiple_of(n * parts * 128, 128), parts * 128)
            rows_out = pl.ds(pl.multiple_of(n * 128, 128), 128)
            moved = jnp.dot(order_ref[...], wraw[rows_in, :], preferred_element_type=F32).astype(BF16)
            for p in range(parts):
                wqkv[rows_out, p * head_dim:(p + 1) * head_dim] = moved[p * 128:(p + 1) * 128]

    gather_order = [(OWN, 0), (LEFT, 0), (RIGHT, 0), (OWN, 1), (LEFT, 1), (RIGHT, 1), (OPP, 0), (OPP, 1)]
    sum_order = [(OPP, 0), (OPP, 1), (RIGHT, 0), (LEFT, 0), (OWN, 0), (RIGHT, 1), (LEFT, 1), (OWN, 1)]
    heads_order = [(OPP, 0), (RIGHT, 0), (LEFT, 0), (OWN, 0), (OPP, 1), (RIGHT, 1), (LEFT, 1), (OWN, 1)]

    def run(order, before, work, after):
        @pl.loop(0, len(order))
        def _(i):
            for n in range(len(order)):
                if n in before:
                    pl.when(i == n)(before[n])
            kind = pick(i, [k for k, _ in order])
            work(pick(i, [s for _, s in order]), pick(i, [chip_of[k] for k, _ in order]), kind)
            for n in range(len(order)):
                if n in after:
                    pl.when(i == n)(after[n])

    def layer_body(layer, _):
        more = layer + 1 < layers

        def arrive(mlp_part):
            def at0():
                gather_mate(0, OWN)

            def at1():
                if mlp_part:
                    pl.when(layer == 0)(lambda: gather_first(0))
                else:
                    gather_first(0)
                gather_second(0)
                gather_mate(0, LEFT)
                gather_mate(0, RIGHT)

            def at3():
                gather_mate(1, OWN)

            def at4():
                gather_first(1)
                gather_second(1)
                if not mlp_part:
                    pl.when(layer > 0)(lambda: wout_collect(layer))
                gather_mate(1, LEFT)
                gather_mate(1, RIGHT)

            def at6():
                if mlp_part:
                    send_near(0)
                gather_third(0)
                gather_mate(0, OPP)

            def at7():
                if mlp_part:
                    send_near(1)
                gather_third(1)
                if mlp_part:
                    send_opp(0)
                else:
                    pl.when(more)(lambda: wout_begin(layer + 1))
                gather_mate(1, OPP)
            return {0: at0, 1: at1, 3: at3, 4: at4, 6: at6, 7: at7}

        def with_fetch(before, stage):
            def act():
                before()
                pl.when(more)(lambda: stage(layer + 1))
            return act

        weight_copy(0, layer).wait()
        sort_wqkv()
        next_weights(layer, (0,))
        run(gather_order, arrive(False), lambda s, d, kind: do_qkv(s, d), {})
        weight_copy(1, layer).wait()

        @pl.when(layer == 0)
        def _():
            def attend_and_project(s, d, kind):
                do_attention(s, d, kind)
                project(s, kind, att.at[s, kind], wout)

            def after3():
                send_near(0)
                send_through(0)

            def after6():
                send_near(1)
                send_through(1)

            run(sum_order, {}, attend_and_project, {
                0: with_fetch(lambda: send_opp(0), wout_pass), 1: lambda: send_opp(1),
                3: with_fetch(after3, wout_share), 6: after6})
            for s in (0, 1):
                finish(s, layer, bo_ref, g2_ref, s2_ref, layer, None)

        @pl.when(layer > 0)
        def _():
            for s in (0, 1):
                for k in (2, 5, 6 + OPP, 6 + RIGHT, 6 + LEFT):
                    gather_copy(s, k).wait_send()
            wout_end(layer)
            for n in range(len(others)):
                wout_load(layer, n).start()

            def with_send(n):
                def act():
                    kind, s = heads_order[n]
                    send_heads(s, kind)
                return act

            def first_rows():
                for n in range(len(others)):
                    wout_load(layer, n).wait()
                finish_attention(0, layer)
                gather_send(0, (0, 3, 6 + OWN))

            after = {n: with_send(n) for n in range(8)}
            if layers > 2:
                after[0] = with_fetch(after[0], wout_pass)
                after[3] = with_fetch(after[3], wout_share)
            send4 = after[4]

            def both4():
                send4()
                first_rows()
            after[4] = both4
            run(heads_order, {}, do_attention, after)
            gather_send(0, (1, 4))
            gather_first(0)
            finish_attention(1, layer)
            gather_send(1)

        next_weights(layer, (1,))

        weight_copy(2, layer).wait()
        weight_copy(3, layer).wait()
        run(gather_order, arrive(True), lambda s, d, kind: do_mlp(s, d, kind, layer), {})
        next_weights(layer, (2, 3))
        send_opp(1)
        send_through(0)
        send_through(1)
        last = layer == layers - 1
        for s in (0, 1):
            finish(s, layer, bd_ref, g1_ref, s1_ref, jnp.minimum(layer + 1, layers - 1), last)
        return 0

    lax.fori_loop(0, layers, layer_body, 0)


def solution(mesh):
    tp_size = mesh.shape["tp"]
    sharers = math.gcd(mesh.shape["dp"], 4)

    def local_forward(x_local, ln1_gain, ln1_bias, ln2_gain, ln2_bias, w_qkv, w_out, b_out, w_up, b_up, w_down, b_down):
        batch, rows, width = x_local.shape
        layers, _, _, heads, head_dim = w_qkv.shape
        hidden = w_up.shape[2]
        hd = heads * head_dim
        chips = tp_size // 2
        half, quarter = rows // 2, rows // 4
        vmem = pl.BlockSpec(memory_space=pltpu.VMEM)
        anywhere = pl.BlockSpec(memory_space=pl.ANY)
        call = pl.pallas_call(
            functools.partial(decoder, tp_size, sharers, layers, heads, head_dim),
            out_shape=(jax.ShapeDtypeStruct((rows, width), BF16), jax.ShapeDtypeStruct((layers, tp_size, hd, width), BF16)),
            in_specs=[vmem] * 8 + [anywhere] * 4,
            out_specs=(vmem, anywhere),
            scratch_shapes=[
                pltpu.VMEM((chips, 2, rows, width), BF16),
                pltpu.VMEM((chips, 2 * rows, 2 * hd), BF16),
                pltpu.VMEM((chips, hd, 2 * rows), BF16),
                pltpu.VMEM((rows, width), F32),
                pltpu.VMEM((2, 4, half, width), F32),
                pltpu.VMEM((max(8 * half, 4 * hd), width), BF16),
                pltpu.VMEM((2, 4, half, width), BF16),
                pltpu.VMEM((max(12 * quarter, 3 * hd), width), BF16),
                pltpu.VMEM((2, 6, quarter, width), BF16),
                pltpu.VMEM((heads, chips, 2 * rows, rows), F32),
                pltpu.VMEM((2, 2 * rows, rows), F32),
                pltpu.VMEM((rows, hidden), BF16),
                pltpu.VMEM((2, 4, rows, hd), BF16),
                pltpu.VMEM((2, half, tp_size * hd), BF16),
                pltpu.VMEM((3 * heads * width, head_dim), BF16),
                pltpu.VMEM((3 * heads * 128, 3 * heads * 128), BF16),
                pltpu.VMEM((width, 3 * hd), BF16),
                pltpu.VMEM((hd, width), BF16),
                pltpu.VMEM((width, hidden), BF16),
                pltpu.VMEM((hidden, width), BF16),
                pltpu.SemaphoreType.DMA((4,)),
                pltpu.SemaphoreType.DMA((7,)),
                pltpu.SemaphoreType.DMA((2, 10)),
                pltpu.SemaphoreType.DMA((2, 10)),
                pltpu.SemaphoreType.DMA((2, 10)),
                pltpu.SemaphoreType.DMA((2, 10)),
                pltpu.SemaphoreType.DMA((2, 8)),
                pltpu.SemaphoreType.DMA((2, 8)),
                pltpu.SemaphoreType.DMA((layers, 7 + 3 * sharers)),
                pltpu.SemaphoreType.DMA((layers, 7 + 3 * sharers)),
            ],
            compiler_params=pltpu.CompilerParams(collective_id=0, has_side_effects=True, vmem_limit_bytes=64 * 1024 * 1024 - 128 * 1024),
        )
        y, _ = call(
            x_local.reshape(rows, width), ln1_gain, ln1_bias, ln2_gain, ln2_bias, b_out, b_up, b_down,
            w_qkv.reshape(layers, width * 3 * heads, head_dim), w_out.reshape(layers, hd, width), w_up, w_down,
        )
        return y.reshape(batch, rows, width)

    rows_spec = P("dp", "tp", None)
    in_specs = (rows_spec, P(), P(), P(), P(), P(None, None, None, "tp", None), P(None, "tp", None, None), P(), P(None, None, "tp"), P(None, "tp"), P(None, "tp", None), P())
    return jax.shard_map(local_forward, mesh=mesh, in_specs=in_specs, out_specs=rows_spec, check_vma=False)
```

```python
import functools
import math
import jax
import jax.numpy as jnp
from jax import lax
from jax.experimental import pallas as pl
from jax.experimental.pallas import tpu as pltpu
from jax.sharding import PartitionSpec as P

F32 = jnp.float32
BF16 = jnp.bfloat16
MESH = pl.DeviceIdType.MESH
OPP, RIGHT, LEFT, OWN = range(4)


def pick(i, values):
    out = values[0]
    for n in range(1, len(values)):
        out = jnp.where(i == n, values[n], out)
    return out


def decoder(tp_size, sharers, layers, heads, head_dim,
            x_hbm, g1_ref, s1_ref, g2_ref, s2_ref, bo_ref, bu_ref, bd_ref,
            wqkv_hbm, wout_hbm, wup_hbm, wdown_hbm,
            y_hbm, wg,
            xy, hid, qk, vt, resid, acc, pst, prv, snd, rcv, scores, mask, mlp, att, heads_in,
            wraw, order_ref, wqkv, wout, wup, wdown,
            wsem, lsem, xsem, ysem, ag_ss, ag_rs, rs_ss, rs_rs, hs_ss, hs_rs, wo_ss, wo_rs):
    chips = tp_size // 2
    rows, width = xy.shape
    half, quarter = rows // 2, rows // 4
    hd = heads * head_dim
    scale = 1.0 / math.sqrt(head_dim)
    me = lax.axis_index("tp")
    chip = me // 2
    core = lax.rem(me, 2)
    right = lax.rem(me + 2, tp_size)
    left = lax.rem(me + tp_size - 2, tp_size)
    mate = me + 1 - 2 * core
    opposite = lax.rem(me + tp_size // 2, tp_size)
    group = lax.axis_index("dp")
    side = lax.rem(group, sharers)
    chip_of = [lax.rem(chip + 2, chips), lax.rem(chip + 1, chips), lax.rem(chip + chips - 1, chips), chip]
    top, low = pl.ds(0, quarter), pl.ds(quarter, quarter)
    mine, other = pl.ds(0, half), pl.ds(half, half)

    def x_copy(s):
        return pltpu.make_async_copy(x_hbm.at[pl.ds(s * half, half)], xy.at[pl.ds(s * half, half)], xsem.at[s])

    def y_copy(s):
        return pltpu.make_async_copy(xy.at[pl.ds(s * half, half)], y_hbm.at[pl.ds(s * half, half)], ysem.at[s])

    def remote(src, dst, ss, rs, s, k, to):
        return pltpu.make_async_remote_copy(src, dst, ss.at[s, k], rs.at[s, k], device_id={"tp": to}, device_id_type=MESH)

    def gather_copy(s, k):
        if k < 3:
            blk = hid.at[chip if k < 2 else chip_of[LEFT], s, top if k == 1 else low]
            return remote(blk, blk, ag_ss, ag_rs, s, k, right)
        if k < 6:
            blk = hid.at[chip if k < 5 else chip_of[RIGHT], s, low if k == 4 else top]
            return remote(blk, blk, ag_ss, ag_rs, s, k, left)
        c = chip_of[k - 6]
        return remote(hid.at[c, s, mine], hid.at[c, s, other], ag_ss, ag_rs, s, k, mate)

    part = hd // sharers
    piece = part // 2
    to_mate = 6 + 3 * (sharers - 1)
    wout_copies = to_mate + 4

    def wout_copy(layer, k):
        def rows_at(off, size):
            return pl.ds(pl.multiple_of(side * part + off, piece), size)

        def go(src, dst, to):
            return pltpu.make_async_remote_copy(src, dst, wo_ss.at[layer, k], wo_rs.at[layer, k], device_id=to, device_id_type=MESH)

        if k < 6:
            at = rows_at(piece if k in (0, 2, 4) else 0, piece)
            to = {"tp": right if k < 3 else left}
            if k in (2, 5):
                blk = wg.at[layer, left if k == 2 else right, at]
                return go(blk, blk, to)
            return go(wout_hbm.at[layer, at], wg.at[layer, me, at], to)
        if k < to_mate + 3:
            shard = (left, right, opposite)[k % 3]
            if k < to_mate:
                blk = wg.at[layer, shard, rows_at(0, part)]
                return go(blk, blk, {"dp": group - side + lax.rem(side + (k - 6) // 3 + 1, sharers)})
            return go(wg.at[layer, shard], wg.at[layer, shard], {"tp": mate})
        return go(wout_hbm.at[layer], wg.at[layer, me], {"tp": mate})

    def wout_first(layer):
        for k in (0, 3):
            wout_copy(layer, k).start()

    def wout_second(layer):
        for k in (1, 4):
            wout_copy(layer, k).start()

    def wout_pass(layer):
        for k, onward in ((0, 2), (3, 5)):
            wout_copy(layer, k).wait_recv()
            wout_copy(layer, onward).start()

    def wout_share(layer):
        for k in (1, 4, 2, 5):
            wout_copy(layer, k).wait_recv()
        for k in range(6, to_mate):
            wout_copy(layer, k).start()
        wout_copy(layer, to_mate + 3).start()

    def wout_collect(layer):
        for k in range(6, to_mate):
            wout_copy(layer, k).wait_recv()
        for k in range(to_mate, to_mate + 3):
            wout_copy(layer, k).start()

    def wout_end(layer):
        for k in range(to_mate, wout_copies):
            wout_copy(layer, k).wait_recv()
        for k in range(wout_copies):
            wout_copy(layer, k).wait_send()

    others = [(OPP, 0), (OPP, 1), (LEFT, 0), (LEFT, 1), (RIGHT, 0), (RIGHT, 1), (OWN, 1)]
    seen_from = {OPP: OPP, RIGHT: LEFT, LEFT: RIGHT, OWN: OWN}

    def device_at(kind, across):
        return chip_of[kind] * 2 + (1 - core if across else core)

    def wout_load(layer, n):
        kept = pst.at[pl.ds(n * hd, hd)] if n < 4 else snd.at[pl.ds((n - 4) * hd, hd)]
        return pltpu.make_async_copy(wg.at[layer, device_at(*others[n])], kept, lsem.at[n])

    def heads_copy(s, kind, across):
        slot = 1 + others.index((seen_from[kind], across))
        k = 2 * kind + across
        return pltpu.make_async_remote_copy(
            att.at[s, kind, other if across else mine], heads_in.at[s, :, pl.ds(slot * hd, hd)],
            hs_ss.at[s, k], hs_rs.at[s, k], device_id={"tp": device_at(kind, across)}, device_id_type=MESH)

    def send_heads(s, kind):
        for across in (0, 1):
            if (kind, across) == (OWN, 0):
                heads_in[s, :, :hd] = att[s, OWN, mine, :]
            else:
                heads_copy(s, kind, across).start()

    def gather_send(s, which=(0, 3, 6 + OWN, 1, 4)):
        for k in which:
            gather_copy(s, k).start()

    def gather_first(s):
        gather_copy(s, 0).wait_recv()
        gather_copy(s, 2).start()
        gather_copy(s, 3).wait_recv()
        gather_copy(s, 5).start()

    def gather_second(s):
        gather_copy(s, 1).wait_recv()
        gather_copy(s, 6 + LEFT).start()
        gather_copy(s, 4).wait_recv()
        gather_copy(s, 6 + RIGHT).start()

    def gather_third(s):
        gather_copy(s, 2).wait_recv()
        gather_copy(s, 5).wait_recv()
        gather_copy(s, 6 + OPP).start()

    def gather_mate(s, kind):
        gather_copy(s, 6 + kind).wait_recv()

    def sum_copy(s, k):
        if k < 6:
            return remote(snd.at[pl.ds((s * 6 + k) * quarter, quarter)], rcv.at[s, k], rs_ss, rs_rs, s, k, right if k < 3 else left)
        return remote(pst.at[pl.ds((s * 4 + k - 6) * half, half)], prv.at[s, k - 6], rs_ss, rs_rs, s, k, mate)

    def staged(s, kind):
        return pl.ds(pl.multiple_of((s * 4 + kind) * half, half), half)

    def mate_send(s, kind):
        remote(pst.at[staged(s, kind)], prv.at[s, kind], rs_ss, rs_rs, s, 6 + kind, mate).start()

    step = 16

    def combine(s, kind, r0, dst, extra):
        @pl.loop(0, quarter // step, unroll=True)
        def _(t):
            at = pl.ds(pl.multiple_of(r0 + t * step, step), step)
            at0 = pl.ds(pl.multiple_of(t * step, step), step)
            total = acc[s, kind, at, :] + prv[s, kind, at, :].astype(F32)
            if extra is not None:
                total = total + rcv[s, extra, at0, :].astype(F32)
            snd[pl.ds(pl.multiple_of((s * 6 + dst) * quarter + t * step, step), step), :] = total.astype(BF16)

    def send_opp(s):
        gather_copy(s, 6 + OPP).wait_send()
        sum_copy(s, 6 + OPP).wait_recv()
        combine(s, OPP, quarter, 0, None)
        sum_copy(s, 0).start()
        combine(s, OPP, 0, 3, None)
        sum_copy(s, 3).start()

    def send_near(s):
        sum_copy(s, 6 + RIGHT).wait_recv()
        combine(s, RIGHT, 0, 1, None)
        sum_copy(s, 1).start()
        sum_copy(s, 6 + LEFT).wait_recv()
        combine(s, LEFT, quarter, 4, None)
        sum_copy(s, 4).start()

    def send_through(s):
        for k in (2, 5, 6 + RIGHT, 6 + LEFT):
            gather_copy(s, k).wait_send()
        sum_copy(s, 0).wait_recv()
        combine(s, RIGHT, quarter, 2, 0)
        sum_copy(s, 2).start()
        sum_copy(s, 3).wait_recv()
        combine(s, LEFT, 0, 5, 3)
        sum_copy(s, 5).start()

    def norm_row(s, at0, r, gain_ref, shift_ref, layer):
        mean = jnp.mean(r, axis=-1, keepdims=True)
        centered = r - mean
        var = jnp.mean(centered * centered, axis=-1, keepdims=True)
        normed = centered * lax.rsqrt(var + 1e-5) * gain_ref[pl.ds(layer, 1), :] + shift_ref[pl.ds(layer, 1), :]
        hid[chip, s, at0, :] = normed.astype(BF16)

    def finish(s, layer, bias_ref, gain_ref, shift_ref, next_layer, last):
        for k in (1, 2, 4, 5, 6 + OWN):
            sum_copy(s, k).wait_recv()
        for k in range(10):
            sum_copy(s, k).wait_send()
        for k in (0, 1, 3, 4, 6 + OWN):
            gather_copy(s, k).wait_send()
        for which, a, b in ((0, 1, 5), (1, 2, 4)):
            @pl.loop(0, quarter // step, unroll=True)
            def _(t):
                at0 = pl.ds(pl.multiple_of(t * step, step), step)
                at = pl.ds(pl.multiple_of(which * quarter + t * step, step), step)
                rat = pl.ds(pl.multiple_of(s * half + which * quarter + t * step, step), step)
                total = acc[s, OWN, at, :] + prv[s, OWN, at, :].astype(F32)
                total = total + (rcv[s, a, at0, :].astype(F32) + rcv[s, b, at0, :].astype(F32))
                r = resid[rat, :] + (total + bias_ref[pl.ds(layer, 1), :])
                resid[rat, :] = r
                if last is None:
                    norm_row(s, at, r, gain_ref, shift_ref, next_layer)
                else:
                    @pl.when(last)
                    def _():
                        xy[rat, :] = r.astype(BF16)

                    @pl.when(jnp.logical_not(last))
                    def _():
                        norm_row(s, at, r, gain_ref, shift_ref, next_layer)
        if last is None:
            gather_send(s)
        else:
            @pl.when(last)
            def _():
                y_copy(s).start()

            @pl.when(jnp.logical_not(last))
            def _():
                gather_send(s)

    def finish_attention(s, layer):
        for kind, across in others:
            heads_copy(s, kind, across).wait_recv()
        for kind, across in others:
            heads_copy(s, kind, across).wait_send()
        for k in (0, 1, 3, 4, 6 + OWN):
            gather_copy(s, k).wait_send()
        tile = min(512, width)
        mid = 5 * hd

        @pl.loop(0, width // tile)
        def _(n):
            cols = pl.ds(pl.multiple_of(n * tile, tile), tile)
            total = jnp.dot(heads_in[s, :, :hd], wout[:, cols], preferred_element_type=F32)
            total = total + jnp.dot(heads_in[s, :, hd:mid], pst[:mid - hd, cols], preferred_element_type=F32)
            total = total + jnp.dot(heads_in[s, :, mid:], snd[:tp_size * hd - mid, cols], preferred_element_type=F32)
            at = pl.ds(s * half, half)
            resid[at, cols] = resid[at, cols] + (total + bo_ref[pl.ds(layer, 1), cols])

        @pl.loop(0, half // step, unroll=4)
        def _(t):
            at = pl.ds(pl.multiple_of(t * step, step), step)
            norm_row(s, at, resid[pl.ds(pl.multiple_of(s * half + t * step, step), step), :], g2_ref, s2_ref, layer)

    def block_at(s):
        return pl.ds(pl.multiple_of(s * rows, rows), rows)

    def do_qkv(s, d):
        out = jnp.dot(hid[d, s], wqkv[...], preferred_element_type=F32)
        qk[d, block_at(s), :] = out[:, :2 * hd].astype(BF16)
        vt[d, :, block_at(s)] = jnp.transpose(out[:, 2 * hd:]).astype(BF16)

    def project(s, kind, lhs_ref, w_ref):
        tile = min(1024, width)

        @pl.loop(0, width // tile)
        def _(n):
            cols = pl.ds(pl.multiple_of(n * tile, tile), tile)
            total = jnp.dot(lhs_ref[...], w_ref[:, cols], preferred_element_type=F32)
            acc[s, kind, :, cols] = total[:half]
            pst[staged(s, kind), cols] = total[half:].astype(BF16)
        mate_send(s, kind)

    def do_mlp(s, d, kind, layer):
        hidden = wup.shape[1]
        tile = min(1024, hidden)

        @pl.loop(0, hidden // tile)
        def _(n):
            cols = pl.ds(pl.multiple_of(n * tile, tile), tile)
            pre = jnp.dot(hid[d, s], wup[:, cols], preferred_element_type=F32) + bu_ref[pl.ds(layer, 1), cols]
            mlp[:, cols] = jax.nn.gelu(pre, approximate=True).astype(BF16)
        project(s, kind, mlp, wdown)

    def attend(s, d, kind):
        keys, lanes = 2 * rows, 8
        for h in range(heads):
            at = slice(h * head_dim, (h + 1) * head_dim)
            q = qk[d, block_at(s), at]
            peak = None
            for k in range(d + 1):
                sc = lax.dot_general(qk[k, :, hd + h * head_dim:hd + (h + 1) * head_dim], q, (((1,), (1,)), ((), ())), preferred_element_type=F32)
                if k == d:
                    sc = jnp.where(mask[s] > 0.0, sc, -3e38)
                scores[h, k] = sc
                top_here = jnp.max(sc.reshape(keys // lanes, lanes, rows), axis=0)
                peak = top_here if peak is None else jnp.maximum(peak, top_here)
            peak = jnp.max(peak, axis=0, keepdims=True)
            total = None
            for k in range(d + 1):
                e = jnp.exp2((scores[h, k] - peak) * (scale * math.log2(math.e)))
                scores[h, k] = e
                here = jnp.sum(e.reshape(keys // lanes, lanes, rows), axis=0)
                total = here if total is None else total + here
            inv = 1.0 / jnp.sum(total, axis=0, keepdims=True)
            out = None
            for k in range(d + 1):
                p = (scores[h, k] * inv).astype(BF16)
                here = jnp.dot(vt[k, at, :], p, preferred_element_type=F32)
                out = here if out is None else out + here
            att[s, kind, :, at] = jnp.transpose(out).astype(BF16)

    def do_attention(s, d, kind):
        for n in range(chips):
            @pl.when(d == n)
            def _():
                attend(s, n, kind)

    weights = ((wqkv_hbm, wraw), (wout_hbm, wout), (wup_hbm, wup), (wdown_hbm, wdown))

    def weight_copy(n, layer):
        return pltpu.make_async_copy(weights[n][0].at[layer], weights[n][1], wsem.at[n])

    def next_weights(layer, which):
        @pl.when(layer + 1 < layers)
        def _():
            for n in which:
                weight_copy(n, layer + 1).start()

    barrier = pltpu.get_barrier_semaphore()
    for n in range(1, tp_size):
        pl.semaphore_signal(barrier, inc=1, device_id={"tp": lax.rem(me + n, tp_size)}, device_id_type=MESH)
    for n in range(1, sharers):
        pl.semaphore_signal(barrier, inc=1, device_id={"dp": group - side + lax.rem(side + n, sharers)}, device_id_type=MESH)
    for s in (0, 1):
        x_copy(s).start()
    for n in range(4):
        weight_copy(n, 0).start()
    for s in (0, 1):
        x_copy(s).wait()

        @pl.loop(0, half // step, unroll=4)
        def _(t):
            at = pl.ds(pl.multiple_of(t * step, step), step)
            rat = pl.ds(pl.multiple_of(s * half + t * step, step), step)
            r = xy[rat, :].astype(F32)
            resid[rat, :] = r
            norm_row(s, at, r, g1_ref, s1_ref, 0)
        if s == 0:
            pl.semaphore_wait(barrier, tp_size + sharers - 2)
        gather_send(s)

    key = lax.broadcasted_iota(jnp.int32, (2 * rows, rows), 0)
    key_core = jnp.where(lax.rem(key, rows) < half, core, 1 - core)
    key_at = key_core * rows + jnp.where(key < rows, 0, half) + lax.rem(key, half)
    qry = lax.broadcasted_iota(jnp.int32, (2 * rows, rows), 1)
    qry_at = jnp.where(qry < half, core, 1 - core) * rows + lax.rem(qry, half)
    for s in (0, 1):
        mask[s] = (key_at <= qry_at + s * half).astype(F32)

    parts = 3 * heads
    to = lax.broadcasted_iota(jnp.int32, (parts * 128, parts * 128), 0)
    come = lax.broadcasted_iota(jnp.int32, (parts * 128, parts * 128), 1)
    order_ref[...] = (come == lax.rem(to, 128) * parts + to // 128).astype(BF16)

    def sort_wqkv():
        @pl.loop(0, width // 128)
        def _(n):
            rows_in = pl.ds(pl.multiple_of(n * parts * 128, 128), parts * 128)
            rows_out = pl.ds(pl.multiple_of(n * 128, 128), 128)
            moved = jnp.dot(order_ref[...], wraw[rows_in, :], preferred_element_type=F32).astype(BF16)
            for p in range(parts):
                wqkv[rows_out, p * head_dim:(p + 1) * head_dim] = moved[p * 128:(p + 1) * 128]

    gather_order = [(OWN, 0), (LEFT, 0), (RIGHT, 0), (OWN, 1), (LEFT, 1), (RIGHT, 1), (OPP, 0), (OPP, 1)]
    sum_order = [(OPP, 0), (OPP, 1), (RIGHT, 0), (LEFT, 0), (OWN, 0), (RIGHT, 1), (LEFT, 1), (OWN, 1)]
    heads_order = [(OPP, 0), (RIGHT, 0), (LEFT, 0), (OWN, 0), (OPP, 1), (RIGHT, 1), (LEFT, 1), (OWN, 1)]

    def run(order, before, work, after):
        @pl.loop(0, len(order))
        def _(i):
            for n in range(len(order)):
                if n in before:
                    pl.when(i == n)(before[n])
            kind = pick(i, [k for k, _ in order])
            work(pick(i, [s for _, s in order]), pick(i, [chip_of[k] for k, _ in order]), kind)
            for n in range(len(order)):
                if n in after:
                    pl.when(i == n)(after[n])

    def layer_body(layer, _):
        more = layer + 1 < layers

        def arrive(mlp_part):
            def at0():
                gather_mate(0, OWN)

            def at1():
                if mlp_part:
                    pl.when(layer == 0)(lambda: gather_first(0))
                else:
                    gather_first(0)
                gather_second(0)
                gather_mate(0, LEFT)
                gather_mate(0, RIGHT)

            def at3():
                gather_mate(1, OWN)

            def at4():
                gather_first(1)
                gather_second(1)
                if not mlp_part:
                    pl.when(layer > 0)(lambda: wout_collect(layer))
                gather_mate(1, LEFT)
                gather_mate(1, RIGHT)

            def at6():
                if mlp_part:
                    send_near(0)
                gather_third(0)
                gather_mate(0, OPP)

            def at7():
                if mlp_part:
                    send_near(1)
                gather_third(1)
                if mlp_part:
                    send_opp(0)
                else:
                    @pl.when(more)
                    def _():
                        wout_first(layer + 1)
                        wout_second(layer + 1)
                gather_mate(1, OPP)
            return {0: at0, 1: at1, 3: at3, 4: at4, 6: at6, 7: at7}

        def with_fetch(step_work, stage):
            def act():
                pl.when(more)(lambda: stage(layer + 1))
                step_work()
            return act

        weight_copy(0, layer).wait()
        sort_wqkv()
        next_weights(layer, (0,))
        run(gather_order, arrive(False), lambda s, d, kind: do_qkv(s, d), {})
        weight_copy(1, layer).wait()

        @pl.when(layer == 0)
        def _():
            def attend_and_project(s, d, kind):
                do_attention(s, d, kind)
                project(s, kind, att.at[s, kind], wout)

            def after3():
                send_near(0)
                send_through(0)

            def after6():
                send_near(1)
                send_through(1)

            run(sum_order, {}, attend_and_project, {
                0: with_fetch(lambda: send_opp(0), wout_pass), 1: lambda: send_opp(1),
                3: with_fetch(after3, wout_share), 6: after6})
            for s in (0, 1):
                finish(s, layer, bo_ref, g2_ref, s2_ref, layer, None)

        @pl.when(layer > 0)
        def _():
            for s in (0, 1):
                for k in (2, 5, 6 + OPP, 6 + RIGHT, 6 + LEFT):
                    gather_copy(s, k).wait_send()
            wout_end(layer)
            for n in range(len(others)):
                wout_load(layer, n).start()

            def with_send(n):
                def act():
                    kind, s = heads_order[n]
                    send_heads(s, kind)
                return act

            def first_rows():
                for n in range(len(others)):
                    wout_load(layer, n).wait()
                finish_attention(0, layer)
                gather_send(0, (0, 3, 6 + OWN))

            after = {n: with_send(n) for n in range(8)}
            if layers > 2:
                after[1] = with_fetch(after[1], wout_pass)
                after[5] = with_fetch(after[5], wout_share)
            send4 = after[4]

            def both4():
                send4()
                first_rows()
            after[4] = both4
            run(heads_order, {}, do_attention, after)
            gather_send(0, (1, 4))
            gather_first(0)
            finish_attention(1, layer)
            gather_send(1)

        next_weights(layer, (1,))

        weight_copy(2, layer).wait()
        weight_copy(3, layer).wait()
        run(gather_order, arrive(True), lambda s, d, kind: do_mlp(s, d, kind, layer), {})
        next_weights(layer, (2, 3))
        send_opp(1)
        send_through(0)
        send_through(1)
        last = layer == layers - 1
        for s in (0, 1):
            finish(s, layer, bd_ref, g1_ref, s1_ref, jnp.minimum(layer + 1, layers - 1), last)
        return 0

    lax.fori_loop(0, layers, layer_body, 0)
    for s in (0, 1):
        y_copy(s).wait()


def solution(mesh):
    tp_size = mesh.shape["tp"]
    sharers = math.gcd(mesh.shape["dp"], 4)

    def local_forward(x_local, ln1_gain, ln1_bias, ln2_gain, ln2_bias, w_qkv, w_out, b_out, w_up, b_up, w_down, b_down):
        batch, rows, width = x_local.shape
        layers, _, _, heads, head_dim = w_qkv.shape
        hidden = w_up.shape[2]
        hd = heads * head_dim
        chips = tp_size // 2
        half, quarter = rows // 2, rows // 4
        vmem = pl.BlockSpec(memory_space=pltpu.VMEM)
        anywhere = pl.BlockSpec(memory_space=pl.ANY)
        call = pl.pallas_call(
            functools.partial(decoder, tp_size, sharers, layers, heads, head_dim),
            out_shape=(jax.ShapeDtypeStruct((rows, width), BF16), jax.ShapeDtypeStruct((layers, tp_size, hd, width), BF16)),
            in_specs=[anywhere] + [vmem] * 7 + [anywhere] * 4,
            out_specs=(anywhere, anywhere),
            scratch_shapes=[
                pltpu.VMEM((rows, width), BF16),
                pltpu.VMEM((chips, 2, rows, width), BF16),
                pltpu.VMEM((chips, 2 * rows, 2 * hd), BF16),
                pltpu.VMEM((chips, hd, 2 * rows), BF16),
                pltpu.VMEM((rows, width), F32),
                pltpu.VMEM((2, 4, half, width), F32),
                pltpu.VMEM((max(8 * half, 4 * hd), width), BF16),
                pltpu.VMEM((2, 4, half, width), BF16),
                pltpu.VMEM((max(12 * quarter, 3 * hd), width), BF16),
                pltpu.VMEM((2, 6, quarter, width), BF16),
                pltpu.VMEM((heads, chips, 2 * rows, rows), F32),
                pltpu.VMEM((2, 2 * rows, rows), F32),
                pltpu.VMEM((rows, hidden), BF16),
                pltpu.VMEM((2, 4, rows, hd), BF16),
                pltpu.VMEM((2, half, tp_size * hd), BF16),
                pltpu.VMEM((3 * heads * width, head_dim), BF16),
                pltpu.VMEM((3 * heads * 128, 3 * heads * 128), BF16),
                pltpu.VMEM((width, 3 * hd), BF16),
                pltpu.VMEM((hd, width), BF16),
                pltpu.VMEM((width, hidden), BF16),
                pltpu.VMEM((hidden, width), BF16),
                pltpu.SemaphoreType.DMA((4,)),
                pltpu.SemaphoreType.DMA((7,)),
                pltpu.SemaphoreType.DMA((2,)),
                pltpu.SemaphoreType.DMA((2,)),
                pltpu.SemaphoreType.DMA((2, 10)),
                pltpu.SemaphoreType.DMA((2, 10)),
                pltpu.SemaphoreType.DMA((2, 10)),
                pltpu.SemaphoreType.DMA((2, 10)),
                pltpu.SemaphoreType.DMA((2, 8)),
                pltpu.SemaphoreType.DMA((2, 8)),
                pltpu.SemaphoreType.DMA((layers, 7 + 3 * sharers)),
                pltpu.SemaphoreType.DMA((layers, 7 + 3 * sharers)),
            ],
            compiler_params=pltpu.CompilerParams(collective_id=0, has_side_effects=True, vmem_limit_bytes=64 * 1024 * 1024 - 128 * 1024),
        )
        y, _ = call(
            x_local.reshape(rows, width), ln1_gain, ln1_bias, ln2_gain, ln2_bias, b_out, b_up, b_down,
            w_qkv.reshape(layers, width * 3 * heads, head_dim), w_out.reshape(layers, hd, width), w_up, w_down,
        )
        return y.reshape(batch, rows, width)

    rows_spec = P("dp", "tp", None)
    in_specs = (rows_spec, P(), P(), P(), P(), P(None, None, None, "tp", None), P(None, "tp", None, None), P(), P(None, None, "tp"), P(None, "tp"), P(None, "tp", None), P())
    return jax.shard_map(local_forward, mesh=mesh, in_specs=in_specs, out_specs=rows_spec, check_vma=False)
```

```python
import functools
import math
import jax
import jax.numpy as jnp
from jax import lax
from jax.experimental import pallas as pl
from jax.experimental.pallas import tpu as pltpu
from jax.sharding import PartitionSpec as P

F32 = jnp.float32
BF16 = jnp.bfloat16
MESH = pl.DeviceIdType.MESH
OPP, RIGHT, LEFT, OWN = range(4)


def pick(i, values):
    out = values[0]
    for n in range(1, len(values)):
        out = jnp.where(i == n, values[n], out)
    return out


def decoder(tp_size, sharers, layers, heads, head_dim,
            x_hbm, g1_ref, s1_ref, g2_ref, s2_ref, bo_ref, bu_ref, bd_ref,
            wqkv_hbm, wout_hbm, wup_hbm, wdown_hbm,
            y_hbm, wg,
            xy, hid, qk, vt, resid, acc, pst, prv, snd, rcv, scores, mask, mlp, att, heads_in,
            wraw, order_ref, wqkv, wout, wup, wdown,
            wsem, lsem, xsem, ysem, ag_ss, ag_rs, rs_ss, rs_rs, hs_ss, hs_rs, wo_ss, wo_rs):
    chips = tp_size // 2
    rows, width = xy.shape
    half, quarter = rows // 2, rows // 4
    hd = heads * head_dim
    scale = 1.0 / math.sqrt(head_dim)
    me = lax.axis_index("tp")
    chip = me // 2
    core = lax.rem(me, 2)
    right = lax.rem(me + 2, tp_size)
    left = lax.rem(me + tp_size - 2, tp_size)
    mate = me + 1 - 2 * core
    opposite = lax.rem(me + tp_size // 2, tp_size)
    group = lax.axis_index("dp")
    side = lax.rem(group, sharers)
    chip_of = [lax.rem(chip + 2, chips), lax.rem(chip + 1, chips), lax.rem(chip + chips - 1, chips), chip]
    top, low = pl.ds(0, quarter), pl.ds(quarter, quarter)
    mine, other = pl.ds(0, half), pl.ds(half, half)

    def x_copy(s):
        return pltpu.make_async_copy(x_hbm.at[pl.ds(s * half, half)], xy.at[pl.ds(s * half, half)], xsem.at[s])

    def y_copy(s):
        return pltpu.make_async_copy(xy.at[pl.ds(s * half, half)], y_hbm.at[pl.ds(s * half, half)], ysem.at[s])

    def remote(src, dst, ss, rs, s, k, to):
        return pltpu.make_async_remote_copy(src, dst, ss.at[s, k], rs.at[s, k], device_id={"tp": to}, device_id_type=MESH)

    def gather_copy(s, k):
        if k < 3:
            blk = hid.at[chip if k < 2 else chip_of[LEFT], s, top if k == 1 else low]
            return remote(blk, blk, ag_ss, ag_rs, s, k, right)
        if k < 6:
            blk = hid.at[chip if k < 5 else chip_of[RIGHT], s, low if k == 4 else top]
            return remote(blk, blk, ag_ss, ag_rs, s, k, left)
        c = chip_of[k - 6]
        return remote(hid.at[c, s, mine], hid.at[c, s, other], ag_ss, ag_rs, s, k, mate)

    part = hd // sharers
    piece = part // 2
    to_mate = 6 + 3 * (sharers - 1)
    wout_copies = to_mate + 4

    def wout_copy(layer, k):
        def rows_at(off, size):
            return pl.ds(pl.multiple_of(side * part + off, piece), size)

        def go(src, dst, to):
            return pltpu.make_async_remote_copy(src, dst, wo_ss.at[layer, k], wo_rs.at[layer, k], device_id=to, device_id_type=MESH)

        if k < 6:
            at = rows_at(piece if k in (0, 2, 4) else 0, piece)
            to = {"tp": right if k < 3 else left}
            if k in (2, 5):
                blk = wg.at[layer, left if k == 2 else right, at]
                return go(blk, blk, to)
            return go(wout_hbm.at[layer, at], wg.at[layer, me, at], to)
        if k < to_mate + 3:
            shard = (left, right, opposite)[k % 3]
            if k < to_mate:
                blk = wg.at[layer, shard, rows_at(0, part)]
                return go(blk, blk, {"dp": group - side + lax.rem(side + (k - 6) // 3 + 1, sharers)})
            return go(wg.at[layer, shard], wg.at[layer, shard], {"tp": mate})
        return go(wout_hbm.at[layer], wg.at[layer, me], {"tp": mate})

    def wout_first(layer):
        for k in (0, 3):
            wout_copy(layer, k).start()

    def wout_second(layer):
        for k in (1, 4):
            wout_copy(layer, k).start()

    def wout_pass(layer):
        for k, onward in ((0, 2), (3, 5)):
            wout_copy(layer, k).wait_recv()
            wout_copy(layer, onward).start()

    def wout_share(layer):
        for k in (1, 4, 2, 5):
            wout_copy(layer, k).wait_recv()
        for k in range(6, to_mate):
            wout_copy(layer, k).start()
        wout_copy(layer, to_mate + 3).start()

    def wout_collect(layer):
        for k in range(6, to_mate):
            wout_copy(layer, k).wait_recv()
        for k in range(to_mate, to_mate + 3):
            wout_copy(layer, k).start()

    def wout_end(layer):
        for k in range(to_mate, wout_copies):
            wout_copy(layer, k).wait_recv()
        for k in range(wout_copies):
            wout_copy(layer, k).wait_send()

    others = [(OPP, 0), (OPP, 1), (LEFT, 0), (LEFT, 1), (RIGHT, 0), (RIGHT, 1), (OWN, 1)]
    seen_from = {OPP: OPP, RIGHT: LEFT, LEFT: RIGHT, OWN: OWN}

    def device_at(kind, across):
        return chip_of[kind] * 2 + (1 - core if across else core)

    def wout_load(layer, n):
        kept = pst.at[pl.ds(n * hd, hd)] if n < 4 else snd.at[pl.ds((n - 4) * hd, hd)]
        return pltpu.make_async_copy(wg.at[layer, device_at(*others[n])], kept, lsem.at[n])

    def heads_copy(s, kind, across):
        slot = 1 + others.index((seen_from[kind], across))
        k = 2 * kind + across
        return pltpu.make_async_remote_copy(
            att.at[s, kind, other if across else mine], heads_in.at[s, :, pl.ds(slot * hd, hd)],
            hs_ss.at[s, k], hs_rs.at[s, k], device_id={"tp": device_at(kind, across)}, device_id_type=MESH)

    def send_heads(s, kind):
        for across in (0, 1):
            if (kind, across) == (OWN, 0):
                heads_in[s, :, :hd] = att[s, OWN, mine, :]
            else:
                heads_copy(s, kind, across).start()

    def gather_send(s, which=(0, 3, 6 + OWN, 1, 4)):
        for k in which:
            gather_copy(s, k).start()

    def gather_first(s):
        gather_copy(s, 0).wait_recv()
        gather_copy(s, 2).start()
        gather_copy(s, 3).wait_recv()
        gather_copy(s, 5).start()

    def gather_second(s):
        gather_copy(s, 1).wait_recv()
        gather_copy(s, 6 + LEFT).start()
        gather_copy(s, 4).wait_recv()
        gather_copy(s, 6 + RIGHT).start()

    def gather_third(s):
        gather_copy(s, 2).wait_recv()
        gather_copy(s, 5).wait_recv()
        gather_copy(s, 6 + OPP).start()

    def gather_mate(s, kind):
        gather_copy(s, 6 + kind).wait_recv()

    def sum_copy(s, k):
        if k < 6:
            return remote(snd.at[pl.ds((s * 6 + k) * quarter, quarter)], rcv.at[s, k], rs_ss, rs_rs, s, k, right if k < 3 else left)
        return remote(pst.at[pl.ds((s * 4 + k - 6) * half, half)], prv.at[s, k - 6], rs_ss, rs_rs, s, k, mate)

    def staged(s, kind):
        return pl.ds(pl.multiple_of((s * 4 + kind) * half, half), half)

    def mate_send(s, kind):
        remote(pst.at[staged(s, kind)], prv.at[s, kind], rs_ss, rs_rs, s, 6 + kind, mate).start()

    step = 16

    def combine(s, kind, r0, dst, extra):
        @pl.loop(0, quarter // step, unroll=True)
        def _(t):
            at = pl.ds(pl.multiple_of(r0 + t * step, step), step)
            at0 = pl.ds(pl.multiple_of(t * step, step), step)
            total = acc[s, kind, at, :] + prv[s, kind, at, :].astype(F32)
            if extra is not None:
                total = total + rcv[s, extra, at0, :].astype(F32)
            snd[pl.ds(pl.multiple_of((s * 6 + dst) * quarter + t * step, step), step), :] = total.astype(BF16)

    def send_opp(s):
        gather_copy(s, 6 + OPP).wait_send()
        sum_copy(s, 6 + OPP).wait_recv()
        combine(s, OPP, quarter, 0, None)
        sum_copy(s, 0).start()
        combine(s, OPP, 0, 3, None)
        sum_copy(s, 3).start()

    def send_near(s):
        sum_copy(s, 6 + RIGHT).wait_recv()
        combine(s, RIGHT, 0, 1, None)
        sum_copy(s, 1).start()
        sum_copy(s, 6 + LEFT).wait_recv()
        combine(s, LEFT, quarter, 4, None)
        sum_copy(s, 4).start()

    def send_through(s):
        for k in (2, 5, 6 + RIGHT, 6 + LEFT):
            gather_copy(s, k).wait_send()
        sum_copy(s, 0).wait_recv()
        combine(s, RIGHT, quarter, 2, 0)
        sum_copy(s, 2).start()
        sum_copy(s, 3).wait_recv()
        combine(s, LEFT, 0, 5, 3)
        sum_copy(s, 5).start()

    def norm_row(s, at0, r, gain_ref, shift_ref, layer):
        mean = jnp.mean(r, axis=-1, keepdims=True)
        centered = r - mean
        var = jnp.mean(centered * centered, axis=-1, keepdims=True)
        normed = centered * lax.rsqrt(var + 1e-5) * gain_ref[pl.ds(layer, 1), :] + shift_ref[pl.ds(layer, 1), :]
        hid[chip, s, at0, :] = normed.astype(BF16)

    def finish(s, layer, bias_ref, gain_ref, shift_ref, next_layer, last):
        for k in (1, 2, 4, 5, 6 + OWN):
            sum_copy(s, k).wait_recv()
        for k in range(10):
            sum_copy(s, k).wait_send()
        for k in (0, 1, 3, 4, 6 + OWN):
            gather_copy(s, k).wait_send()
        def new_rows(use):
            for which, a, b in ((0, 1, 5), (1, 2, 4)):
                @pl.loop(0, quarter // step, unroll=True)
                def _(t):
                    at0 = pl.ds(pl.multiple_of(t * step, step), step)
                    at = pl.ds(pl.multiple_of(which * quarter + t * step, step), step)
                    rat = pl.ds(pl.multiple_of(s * half + which * quarter + t * step, step), step)
                    total = acc[s, OWN, at, :] + prv[s, OWN, at, :].astype(F32)
                    total = total + (rcv[s, a, at0, :].astype(F32) + rcv[s, b, at0, :].astype(F32))
                    use(at, rat, resid[rat, :] + (total + bias_ref[pl.ds(layer, 1), :]))

        def keep_and_norm(at, rat, r):
            resid[rat, :] = r
            norm_row(s, at, r, gain_ref, shift_ref, next_layer)

        def go_on():
            new_rows(keep_and_norm)
            gather_send(s)

        def write(at, rat, r):
            xy[rat, :] = r.astype(BF16)

        if last is None:
            go_on()
        else:
            @pl.when(last)
            def _():
                new_rows(write)
                y_copy(s).start()

            pl.when(jnp.logical_not(last))(go_on)

    def finish_attention(s, layer):
        for kind, across in others:
            heads_copy(s, kind, across).wait_recv()
        for kind, across in others:
            heads_copy(s, kind, across).wait_send()
        for k in (0, 1, 3, 4, 6 + OWN):
            gather_copy(s, k).wait_send()
        tile = min(512, width)
        mid = 5 * hd

        @pl.loop(0, width // tile)
        def _(n):
            cols = pl.ds(pl.multiple_of(n * tile, tile), tile)
            total = jnp.dot(heads_in[s, :, :hd], wout[:, cols], preferred_element_type=F32)
            total = total + jnp.dot(heads_in[s, :, hd:mid], pst[:mid - hd, cols], preferred_element_type=F32)
            total = total + jnp.dot(heads_in[s, :, mid:], snd[:tp_size * hd - mid, cols], preferred_element_type=F32)
            at = pl.ds(s * half, half)
            resid[at, cols] = resid[at, cols] + (total + bo_ref[pl.ds(layer, 1), cols])

        @pl.loop(0, half // step, unroll=4)
        def _(t):
            at = pl.ds(pl.multiple_of(t * step, step), step)
            norm_row(s, at, resid[pl.ds(pl.multiple_of(s * half + t * step, step), step), :], g2_ref, s2_ref, layer)

    def block_at(s):
        return pl.ds(pl.multiple_of(s * rows, rows), rows)

    def do_qkv(s, d):
        out = jnp.dot(hid[d, s], wqkv[...], preferred_element_type=F32)
        qk[d, block_at(s), :] = out[:, :2 * hd].astype(BF16)
        vt[d, :, block_at(s)] = jnp.transpose(out[:, 2 * hd:]).astype(BF16)

    def project(s, kind, lhs_ref, w_ref):
        tile = min(1024, width)

        @pl.loop(0, width // tile)
        def _(n):
            cols = pl.ds(pl.multiple_of(n * tile, tile), tile)
            total = jnp.dot(lhs_ref[...], w_ref[:, cols], preferred_element_type=F32)
            acc[s, kind, :, cols] = total[:half]
            pst[staged(s, kind), cols] = total[half:].astype(BF16)
        mate_send(s, kind)

    def do_mlp(s, d, kind, layer):
        hidden = wup.shape[1]
        tile = min(1024, hidden)

        @pl.loop(0, hidden // tile)
        def _(n):
            cols = pl.ds(pl.multiple_of(n * tile, tile), tile)
            pre = jnp.dot(hid[d, s], wup[:, cols], preferred_element_type=F32) + bu_ref[pl.ds(layer, 1), cols]
            mlp[:, cols] = jax.nn.gelu(pre, approximate=True).astype(BF16)
        project(s, kind, mlp, wdown)

    def attend(s, d, kind):
        keys, lanes = 2 * rows, 8
        for h in range(heads):
            at = slice(h * head_dim, (h + 1) * head_dim)
            q = qk[d, block_at(s), at]
            peak = None
            for k in range(d + 1):
                sc = lax.dot_general(qk[k, :, hd + h * head_dim:hd + (h + 1) * head_dim], q, (((1,), (1,)), ((), ())), preferred_element_type=F32)
                if k == d:
                    sc = jnp.where(mask[s] > 0.0, sc, -3e38)
                scores[h, k] = sc
                top_here = jnp.max(sc.reshape(keys // lanes, lanes, rows), axis=0)
                peak = top_here if peak is None else jnp.maximum(peak, top_here)
            peak = jnp.max(peak, axis=0, keepdims=True)
            total = None
            for k in range(d + 1):
                e = jnp.exp2((scores[h, k] - peak) * (scale * math.log2(math.e)))
                scores[h, k] = e
                here = jnp.sum(e.reshape(keys // lanes, lanes, rows), axis=0)
                total = here if total is None else total + here
            inv = 1.0 / jnp.sum(total, axis=0, keepdims=True)
            out = None
            for k in range(d + 1):
                p = (scores[h, k] * inv).astype(BF16)
                here = jnp.dot(vt[k, at, :], p, preferred_element_type=F32)
                out = here if out is None else out + here
            att[s, kind, :, at] = jnp.transpose(out).astype(BF16)

    def do_attention(s, d, kind):
        for n in range(chips):
            @pl.when(d == n)
            def _():
                attend(s, n, kind)

    weights = ((wqkv_hbm, wraw), (wout_hbm, wout), (wup_hbm, wup), (wdown_hbm, wdown))

    def weight_copy(n, layer):
        return pltpu.make_async_copy(weights[n][0].at[layer], weights[n][1], wsem.at[n])

    def next_weights(layer, which):
        @pl.when(layer + 1 < layers)
        def _():
            for n in which:
                weight_copy(n, layer + 1).start()

    barrier = pltpu.get_barrier_semaphore()
    for n in range(1, tp_size):
        pl.semaphore_signal(barrier, inc=1, device_id={"tp": lax.rem(me + n, tp_size)}, device_id_type=MESH)
    for n in range(1, sharers):
        pl.semaphore_signal(barrier, inc=1, device_id={"dp": group - side + lax.rem(side + n, sharers)}, device_id_type=MESH)
    for s in (0, 1):
        x_copy(s).start()
    for n in range(4):
        weight_copy(n, 0).start()
    for s in (0, 1):
        x_copy(s).wait()

        @pl.loop(0, half // step, unroll=4)
        def _(t):
            at = pl.ds(pl.multiple_of(t * step, step), step)
            rat = pl.ds(pl.multiple_of(s * half + t * step, step), step)
            r = xy[rat, :].astype(F32)
            resid[rat, :] = r
            norm_row(s, at, r, g1_ref, s1_ref, 0)
        if s == 0:
            pl.semaphore_wait(barrier, tp_size + sharers - 2)
        gather_send(s)

    key = lax.broadcasted_iota(jnp.int32, (2 * rows, rows), 0)
    key_core = jnp.where(lax.rem(key, rows) < half, core, 1 - core)
    key_at = key_core * rows + jnp.where(key < rows, 0, half) + lax.rem(key, half)
    qry = lax.broadcasted_iota(jnp.int32, (2 * rows, rows), 1)
    qry_at = jnp.where(qry < half, core, 1 - core) * rows + lax.rem(qry, half)
    for s in (0, 1):
        mask[s] = (key_at <= qry_at + s * half).astype(F32)

    parts = 3 * heads
    to = lax.broadcasted_iota(jnp.int32, (parts * 128, parts * 128), 0)
    come = lax.broadcasted_iota(jnp.int32, (parts * 128, parts * 128), 1)
    order_ref[...] = (come == lax.rem(to, 128) * parts + to // 128).astype(BF16)

    def sort_wqkv():
        @pl.loop(0, width // 128)
        def _(n):
            rows_in = pl.ds(pl.multiple_of(n * parts * 128, 128), parts * 128)
            rows_out = pl.ds(pl.multiple_of(n * 128, 128), 128)
            moved = jnp.dot(order_ref[...], wraw[rows_in, :], preferred_element_type=F32).astype(BF16)
            for p in range(parts):
                wqkv[rows_out, p * head_dim:(p + 1) * head_dim] = moved[p * 128:(p + 1) * 128]

    gather_order = [(OWN, 0), (LEFT, 0), (RIGHT, 0), (OWN, 1), (LEFT, 1), (RIGHT, 1), (OPP, 0), (OPP, 1)]
    sum_order = [(OPP, 0), (OPP, 1), (RIGHT, 0), (LEFT, 0), (OWN, 0), (RIGHT, 1), (LEFT, 1), (OWN, 1)]
    heads_order = [(OPP, 0), (RIGHT, 0), (LEFT, 0), (OWN, 0), (OPP, 1), (RIGHT, 1), (LEFT, 1), (OWN, 1)]

    def run(order, before, work, after):
        @pl.loop(0, len(order))
        def _(i):
            for n in range(len(order)):
                if n in before:
                    pl.when(i == n)(before[n])
            kind = pick(i, [k for k, _ in order])
            work(pick(i, [s for _, s in order]), pick(i, [chip_of[k] for k, _ in order]), kind)
            for n in range(len(order)):
                if n in after:
                    pl.when(i == n)(after[n])

    def layer_body(layer, _):
        more = layer + 1 < layers

        def arrive(mlp_part):
            def at0():
                gather_mate(0, OWN)

            def at1():
                if mlp_part:
                    pl.when(layer == 0)(lambda: gather_first(0))
                else:
                    gather_first(0)
                gather_second(0)
                gather_mate(0, LEFT)
                gather_mate(0, RIGHT)

            def at3():
                gather_mate(1, OWN)

            def at4():
                gather_first(1)
                if mlp_part:
                    send_near(0)
                gather_second(1)
                if not mlp_part:
                    pl.when(layer > 0)(lambda: wout_collect(layer))
                gather_mate(1, LEFT)
                gather_mate(1, RIGHT)

            def at6():
                gather_third(0)
                if mlp_part:
                    send_near(1)
                gather_mate(0, OPP)

            def at7():
                gather_third(1)
                if mlp_part:
                    send_opp(0)
                else:
                    @pl.when(more)
                    def _():
                        wout_first(layer + 1)
                        wout_second(layer + 1)
                gather_mate(1, OPP)
            return {0: at0, 1: at1, 3: at3, 4: at4, 6: at6, 7: at7}

        def with_fetch(step_work, stage):
            def act():
                pl.when(more)(lambda: stage(layer + 1))
                step_work()
            return act

        weight_copy(0, layer).wait()
        sort_wqkv()
        next_weights(layer, (0,))
        run(gather_order, arrive(False), lambda s, d, kind: do_qkv(s, d), {})
        weight_copy(1, layer).wait()

        @pl.when(layer == 0)
        def _():
            def attend_and_project(s, d, kind):
                do_attention(s, d, kind)
                project(s, kind, att.at[s, kind], wout)

            def after3():
                send_near(0)
                send_through(0)

            def after6():
                send_near(1)
                send_through(1)

            run(sum_order, {}, attend_and_project, {
                0: with_fetch(lambda: send_opp(0), wout_pass), 1: lambda: send_opp(1),
                3: with_fetch(after3, wout_share), 6: after6})
            for s in (0, 1):
                finish(s, layer, bo_ref, g2_ref, s2_ref, layer, None)

        @pl.when(layer > 0)
        def _():
            for s in (0, 1):
                for k in (2, 5, 6 + OPP, 6 + RIGHT, 6 + LEFT):
                    gather_copy(s, k).wait_send()
            wout_end(layer)
            for n in range(len(others)):
                wout_load(layer, n).start()

            def with_send(n):
                def act():
                    kind, s = heads_order[n]
                    send_heads(s, kind)
                return act

            def first_rows():
                for n in range(len(others)):
                    wout_load(layer, n).wait()
                finish_attention(0, layer)
                gather_send(0, (0, 3, 6 + OWN))

            after = {n: with_send(n) for n in range(8)}
            if layers > 2:
                after[1] = with_fetch(after[1], wout_pass)
                after[5] = with_fetch(after[5], wout_share)
            send4 = after[4]

            def both4():
                send4()
                first_rows()
            after[4] = both4
            run(heads_order, {}, do_attention, after)
            gather_send(0, (1, 4))
            gather_first(0)
            finish_attention(1, layer)
            gather_send(1)

        next_weights(layer, (1,))

        weight_copy(2, layer).wait()
        weight_copy(3, layer).wait()
        run(gather_order, arrive(True), lambda s, d, kind: do_mlp(s, d, kind, layer), {})
        next_weights(layer, (2, 3))
        send_opp(1)
        send_through(0)
        send_through(1)
        last = layer == layers - 1
        for s in (0, 1):
            finish(s, layer, bd_ref, g1_ref, s1_ref, jnp.minimum(layer + 1, layers - 1), last)
        return 0

    lax.fori_loop(0, layers, layer_body, 0)
    for s in (0, 1):
        y_copy(s).wait()


def solution(mesh):
    tp_size = mesh.shape["tp"]
    sharers = math.gcd(mesh.shape["dp"], 4)

    def local_forward(x_local, ln1_gain, ln1_bias, ln2_gain, ln2_bias, w_qkv, w_out, b_out, w_up, b_up, w_down, b_down):
        batch, rows, width = x_local.shape
        layers, _, _, heads, head_dim = w_qkv.shape
        hidden = w_up.shape[2]
        hd = heads * head_dim
        chips = tp_size // 2
        half, quarter = rows // 2, rows // 4
        vmem = pl.BlockSpec(memory_space=pltpu.VMEM)
        anywhere = pl.BlockSpec(memory_space=pl.ANY)
        call = pl.pallas_call(
            functools.partial(decoder, tp_size, sharers, layers, heads, head_dim),
            out_shape=(jax.ShapeDtypeStruct((rows, width), BF16), jax.ShapeDtypeStruct((layers, tp_size, hd, width), BF16)),
            in_specs=[anywhere] + [vmem] * 7 + [anywhere] * 4,
            out_specs=(anywhere, anywhere),
            scratch_shapes=[
                pltpu.VMEM((rows, width), BF16),
                pltpu.VMEM((chips, 2, rows, width), BF16),
                pltpu.VMEM((chips, 2 * rows, 2 * hd), BF16),
                pltpu.VMEM((chips, hd, 2 * rows), BF16),
                pltpu.VMEM((rows, width), F32),
                pltpu.VMEM((2, 4, half, width), F32),
                pltpu.VMEM((max(8 * half, 4 * hd), width), BF16),
                pltpu.VMEM((2, 4, half, width), BF16),
                pltpu.VMEM((max(12 * quarter, 3 * hd), width), BF16),
                pltpu.VMEM((2, 6, quarter, width), BF16),
                pltpu.VMEM((heads, chips, 2 * rows, rows), F32),
                pltpu.VMEM((2, 2 * rows, rows), F32),
                pltpu.VMEM((rows, hidden), BF16),
                pltpu.VMEM((2, 4, rows, hd), BF16),
                pltpu.VMEM((2, half, tp_size * hd), BF16),
                pltpu.VMEM((3 * heads * width, head_dim), BF16),
                pltpu.VMEM((3 * heads * 128, 3 * heads * 128), BF16),
                pltpu.VMEM((width, 3 * hd), BF16),
                pltpu.VMEM((hd, width), BF16),
                pltpu.VMEM((width, hidden), BF16),
                pltpu.VMEM((hidden, width), BF16),
                pltpu.SemaphoreType.DMA((4,)),
                pltpu.SemaphoreType.DMA((7,)),
                pltpu.SemaphoreType.DMA((2,)),
                pltpu.SemaphoreType.DMA((2,)),
                pltpu.SemaphoreType.DMA((2, 10)),
                pltpu.SemaphoreType.DMA((2, 10)),
                pltpu.SemaphoreType.DMA((2, 10)),
                pltpu.SemaphoreType.DMA((2, 10)),
                pltpu.SemaphoreType.DMA((2, 8)),
                pltpu.SemaphoreType.DMA((2, 8)),
                pltpu.SemaphoreType.DMA((layers, 7 + 3 * sharers)),
                pltpu.SemaphoreType.DMA((layers, 7 + 3 * sharers)),
            ],
            compiler_params=pltpu.CompilerParams(collective_id=0, has_side_effects=True, vmem_limit_bytes=64 * 1024 * 1024 - 128 * 1024),
        )
        y, _ = call(
            x_local.reshape(rows, width), ln1_gain, ln1_bias, ln2_gain, ln2_bias, b_out, b_up, b_down,
            w_qkv.reshape(layers, width * 3 * heads, head_dim), w_out.reshape(layers, hd, width), w_up, w_down,
        )
        return y.reshape(batch, rows, width)

    rows_spec = P("dp", "tp", None)
    in_specs = (rows_spec, P(), P(), P(), P(), P(None, None, None, "tp", None), P(None, "tp", None, None), P(), P(None, None, "tp"), P(None, "tp"), P(None, "tp", None), P())
    return jax.shard_map(local_forward, mesh=mesh, in_specs=in_specs, out_specs=rows_spec, check_vma=False)
```

```python
import functools
import math
import jax
import jax.numpy as jnp
from jax import lax
from jax.experimental import pallas as pl
from jax.experimental.pallas import tpu as pltpu
from jax.sharding import PartitionSpec as P

F32 = jnp.float32
BF16 = jnp.bfloat16
MESH = pl.DeviceIdType.MESH
OPP, RIGHT, LEFT, OWN = range(4)


def pick(i, values):
    out = values[0]
    for n in range(1, len(values)):
        out = jnp.where(i == n, values[n], out)
    return out


def decoder(tp_size, sharers, layers, heads, head_dim,
            x_hbm, g1_ref, s1_ref, g2_ref, s2_ref, bo_ref, bu_ref, bd_ref,
            wqkv_hbm, wout_hbm, wup_hbm, wdown_hbm,
            y_hbm, wg,
            xy, hid, qk, vt, resid, acc, pst, prv, snd, rcv, scores, mask, mlp, att, heads_in,
            wraw, order_ref, wqkv, wout, wup, wdown,
            wsem, lsem, xsem, ysem, ag_ss, ag_rs, rs_ss, rs_rs, hs_ss, hs_rs, wo_ss, wo_rs):
    chips = tp_size // 2
    rows, width = xy.shape
    half, quarter = rows // 2, rows // 4
    hd = heads * head_dim
    scale = 1.0 / math.sqrt(head_dim)
    me = lax.axis_index("tp")
    chip = me // 2
    core = lax.rem(me, 2)
    right = lax.rem(me + 2, tp_size)
    left = lax.rem(me + tp_size - 2, tp_size)
    mate = me + 1 - 2 * core
    opposite = lax.rem(me + tp_size // 2, tp_size)
    group = lax.axis_index("dp")
    side = lax.rem(group, sharers)
    chip_of = [lax.rem(chip + 2, chips), lax.rem(chip + 1, chips), lax.rem(chip + chips - 1, chips), chip]
    top, low = pl.ds(0, quarter), pl.ds(quarter, quarter)
    mine, other = pl.ds(0, half), pl.ds(half, half)

    def x_copy(s):
        return pltpu.make_async_copy(x_hbm.at[pl.ds(s * half, half)], xy.at[pl.ds(s * half, half)], xsem.at[s])

    def y_copy(s):
        return pltpu.make_async_copy(xy.at[pl.ds(s * half, half)], y_hbm.at[pl.ds(s * half, half)], ysem.at[s])

    def remote(src, dst, ss, rs, s, k, to):
        return pltpu.make_async_remote_copy(src, dst, ss.at[s, k], rs.at[s, k], device_id={"tp": to}, device_id_type=MESH)

    def gather_copy(s, k):
        if k < 3:
            blk = hid.at[chip if k < 2 else chip_of[LEFT], s, top if k == 1 else low]
            return remote(blk, blk, ag_ss, ag_rs, s, k, right)
        if k < 6:
            blk = hid.at[chip if k < 5 else chip_of[RIGHT], s, low if k == 4 else top]
            return remote(blk, blk, ag_ss, ag_rs, s, k, left)
        c = chip_of[k - 6]
        return remote(hid.at[c, s, mine], hid.at[c, s, other], ag_ss, ag_rs, s, k, mate)

    part = hd // sharers
    piece = part // 2
    to_mate = 6 + 3 * (sharers - 1)
    wout_copies = to_mate + 4

    def wout_copy(layer, k):
        def rows_at(off, size):
            return pl.ds(pl.multiple_of(side * part + off, piece), size)

        def go(src, dst, to):
            return pltpu.make_async_remote_copy(src, dst, wo_ss.at[layer, k], wo_rs.at[layer, k], device_id=to, device_id_type=MESH)

        if k < 6:
            at = rows_at(piece if k in (0, 2, 4) else 0, piece)
            to = {"tp": right if k < 3 else left}
            if k in (2, 5):
                blk = wg.at[layer, left if k == 2 else right, at]
                return go(blk, blk, to)
            return go(wout_hbm.at[layer, at], wg.at[layer, me, at], to)
        if k < to_mate + 3:
            shard = (left, right, opposite)[k % 3]
            if k < to_mate:
                blk = wg.at[layer, shard, rows_at(0, part)]
                return go(blk, blk, {"dp": group - side + lax.rem(side + (k - 6) // 3 + 1, sharers)})
            return go(wg.at[layer, shard], wg.at[layer, shard], {"tp": mate})
        return go(wout_hbm.at[layer], wg.at[layer, me], {"tp": mate})

    def wout_first(layer):
        for k in (0, 3):
            wout_copy(layer, k).start()

    def wout_second(layer):
        for k in (1, 4):
            wout_copy(layer, k).start()

    def wout_pass(layer):
        for k, onward in ((0, 2), (3, 5)):
            wout_copy(layer, k).wait_recv()
            wout_copy(layer, onward).start()

    def wout_share(layer):
        for k in (1, 4, 2, 5):
            wout_copy(layer, k).wait_recv()
        for k in range(6, to_mate):
            wout_copy(layer, k).start()
        wout_copy(layer, to_mate + 3).start()

    def wout_collect(layer):
        for k in range(6, to_mate):
            wout_copy(layer, k).wait_recv()
        for k in range(to_mate, to_mate + 3):
            wout_copy(layer, k).start()

    def wout_end(layer):
        for k in range(to_mate, wout_copies):
            wout_copy(layer, k).wait_recv()
        for k in range(wout_copies):
            wout_copy(layer, k).wait_send()

    others = [(OPP, 0), (OPP, 1), (LEFT, 0), (LEFT, 1), (RIGHT, 0), (RIGHT, 1), (OWN, 1)]
    seen_from = {OPP: OPP, RIGHT: LEFT, LEFT: RIGHT, OWN: OWN}

    def device_at(kind, across):
        return chip_of[kind] * 2 + (1 - core if across else core)

    def wout_load(layer, n):
        kept = pst.at[pl.ds(n * hd, hd)] if n < 4 else snd.at[pl.ds((n - 4) * hd, hd)]
        return pltpu.make_async_copy(wg.at[layer, device_at(*others[n])], kept, lsem.at[n])

    def heads_copy(s, kind, across):
        slot = 1 + others.index((seen_from[kind], across))
        k = 2 * kind + across
        return pltpu.make_async_remote_copy(
            att.at[s, kind, other if across else mine], heads_in.at[s, :, pl.ds(slot * hd, hd)],
            hs_ss.at[s, k], hs_rs.at[s, k], device_id={"tp": device_at(kind, across)}, device_id_type=MESH)

    def send_heads(s, kind):
        for across in (0, 1):
            if (kind, across) == (OWN, 0):
                heads_in[s, :, :hd] = att[s, OWN, mine, :]
            else:
                heads_copy(s, kind, across).start()

    def gather_send(s, which=(0, 3, 6 + OWN, 1, 4)):
        for k in which:
            gather_copy(s, k).start()

    def gather_first(s):
        gather_copy(s, 0).wait_recv()
        gather_copy(s, 2).start()
        gather_copy(s, 3).wait_recv()
        gather_copy(s, 5).start()

    def gather_second(s):
        gather_copy(s, 1).wait_recv()
        gather_copy(s, 6 + LEFT).start()
        gather_copy(s, 4).wait_recv()
        gather_copy(s, 6 + RIGHT).start()

    def gather_third(s):
        gather_copy(s, 2).wait_recv()
        gather_copy(s, 5).wait_recv()
        gather_copy(s, 6 + OPP).start()

    def gather_mate(s, kind):
        gather_copy(s, 6 + kind).wait_recv()

    def sum_copy(s, k):
        if k < 6:
            return remote(snd.at[pl.ds((s * 6 + k) * quarter, quarter)], rcv.at[s, k], rs_ss, rs_rs, s, k, right if k < 3 else left)
        return remote(pst.at[pl.ds((s * 4 + k - 6) * half, half)], prv.at[s, k - 6], rs_ss, rs_rs, s, k, mate)

    def staged(s, kind):
        return pl.ds(pl.multiple_of((s * 4 + kind) * half, half), half)

    def mate_send(s, kind):
        remote(pst.at[staged(s, kind)], prv.at[s, kind], rs_ss, rs_rs, s, 6 + kind, mate).start()

    step = 16

    def combine(s, kind, r0, dst, extra):
        @pl.loop(0, quarter // step, unroll=True)
        def _(t):
            at = pl.ds(pl.multiple_of(r0 + t * step, step), step)
            at0 = pl.ds(pl.multiple_of(t * step, step), step)
            total = acc[s, kind, at, :] + prv[s, kind, at, :].astype(F32)
            if extra is not None:
                total = total + rcv[s, extra, at0, :].astype(F32)
            snd[pl.ds(pl.multiple_of((s * 6 + dst) * quarter + t * step, step), step), :] = total.astype(BF16)

    def send_opp(s):
        gather_copy(s, 6 + OPP).wait_send()
        sum_copy(s, 6 + OPP).wait_recv()
        combine(s, OPP, quarter, 0, None)
        sum_copy(s, 0).start()
        combine(s, OPP, 0, 3, None)
        sum_copy(s, 3).start()

    def send_near(s):
        sum_copy(s, 6 + RIGHT).wait_recv()
        combine(s, RIGHT, 0, 1, None)
        sum_copy(s, 1).start()
        sum_copy(s, 6 + LEFT).wait_recv()
        combine(s, LEFT, quarter, 4, None)
        sum_copy(s, 4).start()

    def send_through(s):
        for k in (2, 5, 6 + RIGHT, 6 + LEFT):
            gather_copy(s, k).wait_send()
        sum_copy(s, 0).wait_recv()
        combine(s, RIGHT, quarter, 2, 0)
        sum_copy(s, 2).start()
        sum_copy(s, 3).wait_recv()
        combine(s, LEFT, 0, 5, 3)
        sum_copy(s, 5).start()

    def norm_row(s, at0, r, gain_ref, shift_ref, layer):
        mean = jnp.mean(r, axis=-1, keepdims=True)
        centered = r - mean
        var = jnp.mean(centered * centered, axis=-1, keepdims=True)
        normed = centered * lax.rsqrt(var + 1e-5) * gain_ref[pl.ds(layer, 1), :] + shift_ref[pl.ds(layer, 1), :]
        hid[chip, s, at0, :] = normed.astype(BF16)

    def finish(s, layer, bias_ref, gain_ref, shift_ref, next_layer, last):
        for k in (1, 2, 4, 5, 6 + OWN):
            sum_copy(s, k).wait_recv()
        for k in range(10):
            sum_copy(s, k).wait_send()
        for k in (0, 1, 3, 4, 6 + OWN):
            gather_copy(s, k).wait_send()
        def new_rows(use):
            for which, a, b in ((0, 1, 5), (1, 2, 4)):
                @pl.loop(0, quarter // step, unroll=True)
                def _(t):
                    at0 = pl.ds(pl.multiple_of(t * step, step), step)
                    at = pl.ds(pl.multiple_of(which * quarter + t * step, step), step)
                    rat = pl.ds(pl.multiple_of(s * half + which * quarter + t * step, step), step)
                    total = acc[s, OWN, at, :] + prv[s, OWN, at, :].astype(F32)
                    total = total + (rcv[s, a, at0, :].astype(F32) + rcv[s, b, at0, :].astype(F32))
                    use(at, rat, resid[rat, :] + (total + bias_ref[pl.ds(layer, 1), :]))

        def keep_and_norm(at, rat, r):
            resid[rat, :] = r
            norm_row(s, at, r, gain_ref, shift_ref, next_layer)

        def go_on():
            new_rows(keep_and_norm)
            gather_send(s)

        def write(at, rat, r):
            xy[rat, :] = r.astype(BF16)

        if last is None:
            go_on()
        else:
            @pl.when(last)
            def _():
                new_rows(write)
                y_copy(s).start()

            pl.when(jnp.logical_not(last))(go_on)

    def finish_attention(s, layer):
        for kind, across in others:
            heads_copy(s, kind, across).wait_recv()
        for kind, across in others:
            heads_copy(s, kind, across).wait_send()
        for k in (0, 1, 3, 4, 6 + OWN):
            gather_copy(s, k).wait_send()
        tile = min(512, width)
        mid = 5 * hd

        @pl.loop(0, width // tile)
        def _(n):
            cols = pl.ds(pl.multiple_of(n * tile, tile), tile)
            total = jnp.dot(heads_in[s, :, :hd], wout[:, cols], preferred_element_type=F32)
            total = total + jnp.dot(heads_in[s, :, hd:mid], pst[:mid - hd, cols], preferred_element_type=F32)
            total = total + jnp.dot(heads_in[s, :, mid:], snd[:tp_size * hd - mid, cols], preferred_element_type=F32)
            at = pl.ds(s * half, half)
            resid[at, cols] = resid[at, cols] + (total + bo_ref[pl.ds(layer, 1), cols])

        @pl.loop(0, half // step, unroll=4)
        def _(t):
            at = pl.ds(pl.multiple_of(t * step, step), step)
            norm_row(s, at, resid[pl.ds(pl.multiple_of(s * half + t * step, step), step), :], g2_ref, s2_ref, layer)

    def block_at(s):
        return pl.ds(pl.multiple_of(s * rows, rows), rows)

    def do_qkv(s, d):
        out = jnp.dot(hid[d, s], wqkv[...], preferred_element_type=F32)
        qk[d, block_at(s), :] = out[:, :2 * hd].astype(BF16)
        vt[d, :, block_at(s)] = jnp.transpose(out[:, 2 * hd:]).astype(BF16)

    def project(s, kind, lhs_ref, w_ref):
        tile = min(1024, width)

        @pl.loop(0, width // tile)
        def _(n):
            cols = pl.ds(pl.multiple_of(n * tile, tile), tile)
            total = jnp.dot(lhs_ref[...], w_ref[:, cols], preferred_element_type=F32)
            acc[s, kind, :, cols] = total[:half]
            pst[staged(s, kind), cols] = total[half:].astype(BF16)
        mate_send(s, kind)

    def do_mlp(s, d, kind, layer):
        hidden = wup.shape[1]
        tile = min(1024, hidden)

        @pl.loop(0, hidden // tile)
        def _(n):
            cols = pl.ds(pl.multiple_of(n * tile, tile), tile)
            pre = jnp.dot(hid[d, s], wup[:, cols], preferred_element_type=F32) + bu_ref[pl.ds(layer, 1), cols]
            mlp[:, cols] = jax.nn.gelu(pre, approximate=True).astype(BF16)
        project(s, kind, mlp, wdown)

    def attend(s, d, kind):
        keys, lanes = 2 * rows, 8
        for h in range(heads):
            at = slice(h * head_dim, (h + 1) * head_dim)
            q = qk[d, block_at(s), at]
            peak = None
            for k in range(d + 1):
                sc = lax.dot_general(qk[k, :, hd + h * head_dim:hd + (h + 1) * head_dim], q, (((1,), (1,)), ((), ())), preferred_element_type=F32)
                if k == d:
                    sc = jnp.where(mask[s] > 0.0, sc, -3e38)
                scores[h, k] = sc
                top_here = jnp.max(sc.reshape(keys // lanes, lanes, rows), axis=0)
                peak = top_here if peak is None else jnp.maximum(peak, top_here)
            peak = jnp.max(peak, axis=0, keepdims=True)
            total = None
            for k in range(d + 1):
                e = jnp.exp2((scores[h, k] - peak) * (scale * math.log2(math.e)))
                scores[h, k] = e
                here = jnp.sum(e.reshape(keys // lanes, lanes, rows), axis=0)
                total = here if total is None else total + here
            inv = 1.0 / jnp.sum(total, axis=0, keepdims=True)
            out = None
            for k in range(d + 1):
                p = (scores[h, k] * inv).astype(BF16)
                here = jnp.dot(vt[k, at, :], p, preferred_element_type=F32)
                out = here if out is None else out + here
            att[s, kind, :, at] = jnp.transpose(out).astype(BF16)

    def do_attention(s, d, kind):
        for n in range(chips):
            @pl.when(d == n)
            def _():
                attend(s, n, kind)

    weights = ((wqkv_hbm, wraw), (wout_hbm, wout), (wup_hbm, wup), (wdown_hbm, wdown))

    def weight_copy(n, layer):
        return pltpu.make_async_copy(weights[n][0].at[layer], weights[n][1], wsem.at[n])

    def next_weights(layer, which):
        @pl.when(layer + 1 < layers)
        def _():
            for n in which:
                weight_copy(n, layer + 1).start()

    barrier = pltpu.get_barrier_semaphore()
    for n in range(1, tp_size):
        pl.semaphore_signal(barrier, inc=1, device_id={"tp": lax.rem(me + n, tp_size)}, device_id_type=MESH)
    for n in range(1, sharers):
        pl.semaphore_signal(barrier, inc=1, device_id={"dp": group - side + lax.rem(side + n, sharers)}, device_id_type=MESH)
    for s in (0, 1):
        x_copy(s).start()
    for n in range(4):
        weight_copy(n, 0).start()
    for s in (0, 1):
        x_copy(s).wait()

        @pl.loop(0, half // step, unroll=4)
        def _(t):
            at = pl.ds(pl.multiple_of(t * step, step), step)
            rat = pl.ds(pl.multiple_of(s * half + t * step, step), step)
            r = xy[rat, :].astype(F32)
            resid[rat, :] = r
            norm_row(s, at, r, g1_ref, s1_ref, 0)
        if s == 0:
            pl.semaphore_wait(barrier, tp_size + sharers - 2)
        gather_send(s)

    key = lax.broadcasted_iota(jnp.int32, (2 * rows, rows), 0)
    key_core = jnp.where(lax.rem(key, rows) < half, core, 1 - core)
    key_at = key_core * rows + jnp.where(key < rows, 0, half) + lax.rem(key, half)
    qry = lax.broadcasted_iota(jnp.int32, (2 * rows, rows), 1)
    qry_at = jnp.where(qry < half, core, 1 - core) * rows + lax.rem(qry, half)
    for s in (0, 1):
        mask[s] = (key_at <= qry_at + s * half).astype(F32)

    parts = 3 * heads
    to = lax.broadcasted_iota(jnp.int32, (parts * 128, parts * 128), 0)
    come = lax.broadcasted_iota(jnp.int32, (parts * 128, parts * 128), 1)
    order_ref[...] = (come == lax.rem(to, 128) * parts + to // 128).astype(BF16)

    def sort_wqkv():
        @pl.loop(0, width // 128)
        def _(n):
            rows_in = pl.ds(pl.multiple_of(n * parts * 128, 128), parts * 128)
            rows_out = pl.ds(pl.multiple_of(n * 128, 128), 128)
            moved = jnp.dot(order_ref[...], wraw[rows_in, :], preferred_element_type=F32).astype(BF16)
            for p in range(parts):
                wqkv[rows_out, p * head_dim:(p + 1) * head_dim] = moved[p * 128:(p + 1) * 128]

    gather_order = [(OWN, 0), (LEFT, 0), (RIGHT, 0), (OWN, 1), (LEFT, 1), (RIGHT, 1), (OPP, 0), (OPP, 1)]
    sum_order = [(OPP, 0), (OPP, 1), (RIGHT, 0), (LEFT, 0), (OWN, 0), (RIGHT, 1), (LEFT, 1), (OWN, 1)]
    heads_order = [(OPP, 0), (RIGHT, 0), (LEFT, 0), (OWN, 0), (OPP, 1), (RIGHT, 1), (LEFT, 1), (OWN, 1)]

    def run(order, before, work, after):
        @pl.loop(0, len(order))
        def _(i):
            for n in range(len(order)):
                if n in before:
                    pl.when(i == n)(before[n])
            kind = pick(i, [k for k, _ in order])
            work(pick(i, [s for _, s in order]), pick(i, [chip_of[k] for k, _ in order]), kind)
            for n in range(len(order)):
                if n in after:
                    pl.when(i == n)(after[n])

    def layer_body(layer, _):
        more = layer + 1 < layers

        def arrive(mlp_part):
            def at0():
                gather_mate(0, OWN)

            def at1():
                if mlp_part:
                    pl.when(layer == 0)(lambda: gather_first(0))
                else:
                    gather_first(0)
                gather_second(0)
                gather_mate(0, LEFT)
                gather_mate(0, RIGHT)

            def at3():
                gather_mate(1, OWN)

            def at4():
                gather_first(1)
                if mlp_part:
                    send_near(0)
                gather_second(1)
                if not mlp_part:
                    pl.when(layer > 0)(lambda: wout_collect(layer))
                gather_mate(1, LEFT)
                gather_mate(1, RIGHT)

            def at6():
                gather_third(0)
                if mlp_part:
                    send_near(1)
                else:
                    @pl.when(more)
                    def _():
                        wout_first(layer + 1)
                        wout_second(layer + 1)
                gather_mate(0, OPP)

            def at7():
                gather_third(1)
                if mlp_part:
                    send_opp(0)
                gather_mate(1, OPP)
            return {0: at0, 1: at1, 3: at3, 4: at4, 6: at6, 7: at7}

        def with_fetch(step_work, stage):
            def act():
                pl.when(more)(lambda: stage(layer + 1))
                step_work()
            return act

        weight_copy(0, layer).wait()
        sort_wqkv()
        next_weights(layer, (0,))
        run(gather_order, arrive(False), lambda s, d, kind: do_qkv(s, d), {})
        weight_copy(1, layer).wait()

        @pl.when(layer == 0)
        def _():
            def attend_and_project(s, d, kind):
                do_attention(s, d, kind)
                project(s, kind, att.at[s, kind], wout)

            def after3():
                send_near(0)
                send_through(0)

            def after6():
                send_near(1)
                send_through(1)

            run(sum_order, {}, attend_and_project, {
                0: with_fetch(lambda: send_opp(0), wout_pass), 1: lambda: send_opp(1),
                3: with_fetch(after3, wout_share), 6: after6})
            for s in (0, 1):
                finish(s, layer, bo_ref, g2_ref, s2_ref, layer, None)

        @pl.when(layer > 0)
        def _():
            for s in (0, 1):
                for k in (2, 5, 6 + OPP, 6 + RIGHT, 6 + LEFT):
                    gather_copy(s, k).wait_send()
            wout_end(layer)
            for n in range(len(others)):
                wout_load(layer, n).start()

            def with_send(n):
                def act():
                    kind, s = heads_order[n]
                    send_heads(s, kind)
                return act

            def first_rows():
                for n in range(len(others)):
                    wout_load(layer, n).wait()
                finish_attention(0, layer)
                gather_send(0, (0, 3, 6 + OWN))

            after = {n: with_send(n) for n in range(8)}
            if layers > 2:
                after[1] = with_fetch(after[1], wout_pass)
                after[5] = with_fetch(after[5], wout_share)
            send4 = after[4]

            def both4():
                send4()
                first_rows()
            after[4] = both4
            run(heads_order, {}, do_attention, after)
            gather_send(0, (1, 4))
            gather_first(0)
            finish_attention(1, layer)
            gather_send(1)

        next_weights(layer, (1,))

        weight_copy(2, layer).wait()
        weight_copy(3, layer).wait()
        run(gather_order, arrive(True), lambda s, d, kind: do_mlp(s, d, kind, layer), {})
        next_weights(layer, (2, 3))
        send_opp(1)
        send_through(0)
        send_through(1)
        last = layer == layers - 1
        for s in (0, 1):
            finish(s, layer, bd_ref, g1_ref, s1_ref, jnp.minimum(layer + 1, layers - 1), last)
        return 0

    lax.fori_loop(0, layers, layer_body, 0)
    for s in (0, 1):
        y_copy(s).wait()


def solution(mesh):
    tp_size = mesh.shape["tp"]
    sharers = math.gcd(mesh.shape["dp"], 4)

    def local_forward(x_local, ln1_gain, ln1_bias, ln2_gain, ln2_bias, w_qkv, w_out, b_out, w_up, b_up, w_down, b_down):
        batch, rows, width = x_local.shape
        layers, _, _, heads, head_dim = w_qkv.shape
        hidden = w_up.shape[2]
        hd = heads * head_dim
        chips = tp_size // 2
        half, quarter = rows // 2, rows // 4
        vmem = pl.BlockSpec(memory_space=pltpu.VMEM)
        anywhere = pl.BlockSpec(memory_space=pl.ANY)
        call = pl.pallas_call(
            functools.partial(decoder, tp_size, sharers, layers, heads, head_dim),
            out_shape=(jax.ShapeDtypeStruct((rows, width), BF16), jax.ShapeDtypeStruct((layers, tp_size, hd, width), BF16)),
            in_specs=[anywhere] + [vmem] * 7 + [anywhere] * 4,
            out_specs=(anywhere, anywhere),
            scratch_shapes=[
                pltpu.VMEM((rows, width), BF16),
                pltpu.VMEM((chips, 2, rows, width), BF16),
                pltpu.VMEM((chips, 2 * rows, 2 * hd), BF16),
                pltpu.VMEM((chips, hd, 2 * rows), BF16),
                pltpu.VMEM((rows, width), F32),
                pltpu.VMEM((2, 4, half, width), F32),
                pltpu.VMEM((max(8 * half, 4 * hd), width), BF16),
                pltpu.VMEM((2, 4, half, width), BF16),
                pltpu.VMEM((max(12 * quarter, 3 * hd), width), BF16),
                pltpu.VMEM((2, 6, quarter, width), BF16),
                pltpu.VMEM((heads, chips, 2 * rows, rows), F32),
                pltpu.VMEM((2, 2 * rows, rows), F32),
                pltpu.VMEM((rows, hidden), BF16),
                pltpu.VMEM((2, 4, rows, hd), BF16),
                pltpu.VMEM((2, half, tp_size * hd), BF16),
                pltpu.VMEM((3 * heads * width, head_dim), BF16),
                pltpu.VMEM((3 * heads * 128, 3 * heads * 128), BF16),
                pltpu.VMEM((width, 3 * hd), BF16),
                pltpu.VMEM((hd, width), BF16),
                pltpu.VMEM((width, hidden), BF16),
                pltpu.VMEM((hidden, width), BF16),
                pltpu.SemaphoreType.DMA((4,)),
                pltpu.SemaphoreType.DMA((7,)),
                pltpu.SemaphoreType.DMA((2,)),
                pltpu.SemaphoreType.DMA((2,)),
                pltpu.SemaphoreType.DMA((2, 10)),
                pltpu.SemaphoreType.DMA((2, 10)),
                pltpu.SemaphoreType.DMA((2, 10)),
                pltpu.SemaphoreType.DMA((2, 10)),
                pltpu.SemaphoreType.DMA((2, 8)),
                pltpu.SemaphoreType.DMA((2, 8)),
                pltpu.SemaphoreType.DMA((layers, 7 + 3 * sharers)),
                pltpu.SemaphoreType.DMA((layers, 7 + 3 * sharers)),
            ],
            compiler_params=pltpu.CompilerParams(collective_id=0, has_side_effects=True, vmem_limit_bytes=64 * 1024 * 1024 - 128 * 1024),
        )
        y, _ = call(
            x_local.reshape(rows, width), ln1_gain, ln1_bias, ln2_gain, ln2_bias, b_out, b_up, b_down,
            w_qkv.reshape(layers, width * 3 * heads, head_dim), w_out.reshape(layers, hd, width), w_up, w_down,
        )
        return y.reshape(batch, rows, width)

    rows_spec = P("dp", "tp", None)
    in_specs = (rows_spec, P(), P(), P(), P(), P(None, None, None, "tp", None), P(None, "tp", None, None), P(), P(None, None, "tp"), P(None, "tp"), P(None, "tp", None), P())
    return jax.shard_map(local_forward, mesh=mesh, in_specs=in_specs, out_specs=rows_spec, check_vma=False)
```
